32 devices in a mesh: band: 2 (over core), tmpl: 8 (over z, x), tm: 2 (over y).
Axes of the slice: x: 2, y: 2, z: 4, core: 2. Of those that a mesh axis runs over, the one named last changes fastest.
Arguments:
- strain_high: float32 [16384], P('tm'), may hold values from -6 to 6
- strain_mid: float32 [2048], P('tm'), may hold values from -6 to 6
- strain_low: float32 [256], P('tm'), may hold values from -6 to 6
- filters_high: float32 [320, 1024], P('tmpl'), may hold values from -0.1875 to 0.1875
- filters_mid: float32 [320, 1024], P('tmpl'), may hold values from -0.1875 to 0.1875
- filters_low: float32 [320, 128], P('tmpl'), may hold values from -0.5 to 0.5
- recon_high: float32 [320, 2, 2048], P(None, None, 'tmpl'), may hold values from -0.3125 to 0.3125
- recon_mid: float32 [320, 2, 2048], P(None, None, 'tmpl'), may hold values from -0.3125 to 0.3125
- recon_low: float32 [320, 2, 2048], P(None, None, 'tmpl'), may hold values from -0.3125 to 0.3125
- basis_count: int32 [3], replicated, may hold values from 160 to 320
Outputs:
- snr: float32 [2, 2048, 16384], P('band', 'tmpl', 'tm')
The draws below stay inside these ranges and needn't reach their ends.
Inputs may be any that keep to these rules, and one draw needn't show every extreme that they name: basis_count[b] says how many of the first 320 basis vectors band b uses.
All inputs are finite; a program needn't handle non-finite values.
Results may differ from the reference program's by a relative error of at most 0.000082.
Values sent between devices are 32-bit elements; how exact they have to be, the bound alone decides.
A program may use at most 128 MiB of HBM per device.

```python
import jax
import jax.numpy as jnp
from jax import lax

TEMPLATES = 2048
BASIS = 320
TAPS_HIGH = 1024
TAPS_MID = 1024
TAPS_LOW = 128
RATIO = 8
HALF_TAPS = 8
TIME = 16384
N_TMPL = 8


def block_scale(key, dims, cuts, smallest, largest):
    loudness = 1.0
    for dim, blocks in cuts:
        heights = jax.random.uniform(jax.random.fold_in(jax.random.fold_in(key, 6), dim), (blocks,), jnp.float32, smallest / len(cuts), largest / len(cuts))
        loudness = loudness * jnp.repeat(jnp.exp(heights), dims[dim] // blocks).reshape((-1,) + (1,) * (len(dims) - 1 - dim))
    return loudness


def centred(own_key, extent, deviation, limit, split=(), held_as=jnp.bfloat16):
    values = jax.random.normal(own_key, extent, jnp.float32) * deviation
    if len(split) > 0:
        values = block_scale(own_key, extent, split, -0.22, 0.18) * values
    return jnp.clip(values, min=-limit, max=limit).astype(held_as)


def setup_inputs(seed: int = 0) -> dict:
    keys = jax.random.split(jax.random.key(seed), 11)
    return {
        "strain_high": centred(keys[0], (TIME,), 1.0, 6.0, ((0, 2),), jnp.float32),
        "strain_mid": centred(keys[1], (TIME // RATIO,), 1.0, 6.0, ((0, 2),), jnp.float32),
        "strain_low": centred(keys[2], (TIME // (RATIO * RATIO),), 1.0, 6.0, ((0, 2),), jnp.float32),
        "filters_high": centred(keys[3], (BASIS, TAPS_HIGH), TAPS_HIGH ** -0.5, 0.1875, ((0, 8),), jnp.float32),
        "filters_mid": centred(keys[4], (BASIS, TAPS_MID), TAPS_MID ** -0.5, 0.1875, ((0, 8),), jnp.float32),
        "filters_low": centred(keys[5], (BASIS, TAPS_LOW), TAPS_LOW ** -0.5, 0.5, ((0, 8),), jnp.float32),
        "recon_high": centred(keys[6], (BASIS, 2, TEMPLATES), BASIS ** -0.5, 0.3125, ((2, 8),), jnp.float32),
        "recon_mid": centred(keys[7], (BASIS, 2, TEMPLATES), BASIS ** -0.5, 0.3125, ((2, 8),), jnp.float32),
        "recon_low": centred(keys[8], (BASIS, 2, TEMPLATES), BASIS ** -0.5, 0.3125, ((2, 8),), jnp.float32),
        "basis_count": jax.random.randint(keys[9], (3,), BASIS // 2, BASIS + 1).astype(jnp.int32),
    }


highest = lax.Precision.HIGHEST


def interp_value(offset, half_taps):
    return jnp.sinc(offset) * (0.5 + 0.5 * jnp.cos(jnp.pi * offset / (half_taps + 1)))


def interp_table(half_taps):
    phase_frac = jnp.arange(RATIO, dtype=jnp.float32)[:, None] / RATIO
    lag_index = jnp.arange(2 * half_taps, dtype=jnp.float32)[None, :]
    return interp_value(phase_frac - (lag_index - half_taps), half_taps)


def causal(series, filter_rows):
    tap_count = filter_rows.shape[1]
    padded = jnp.concatenate([jnp.zeros((tap_count - 1,), jnp.float32), series])
    result = lax.conv_general_dilated(padded[None, None, :], filter_rows[:, None, ::-1], (1,), "VALID", precision=highest)
    return result[0]


def masked(series, row_limit):
    row_index = jnp.arange(series.shape[0], dtype=jnp.int32)[:, None]
    return jnp.where(row_index < row_limit, series, 0.0)


def contract(weights, series):
    return lax.dot_general(weights, series, (((0,), (0,)), ((), ())), precision=highest, preferred_element_type=jnp.float32)


def upsample(signal, kernel_table):
    half_taps = kernel_table.shape[1] // 2
    channels, sample_count = signal.shape
    padded = jnp.pad(signal, ((0, 0), (half_taps, half_taps)))
    accumulated = jnp.zeros((channels, sample_count, RATIO), jnp.float32)
    for lag_index in range(2 * half_taps):
        accumulated = accumulated + padded[:, lag_index: lag_index + sample_count, None] * kernel_table[None, None, :, lag_index]
    return accumulated.reshape(channels, sample_count * RATIO)


def reference(strain_high, strain_mid, strain_low, filters_high, filters_mid, filters_low, recon_high, recon_mid, recon_low, basis_count):
    series_high = masked(causal(strain_high, filters_high), basis_count[0])
    series_mid = masked(causal(strain_mid, filters_mid), basis_count[1])
    series_low = masked(causal(strain_low, filters_low), basis_count[2])
    kernel_table = interp_table(HALF_TAPS)
    block_tmpl = TEMPLATES // N_TMPL
    starts = (jnp.arange(N_TMPL, dtype=jnp.int32) * block_tmpl).astype(jnp.int32)

    def one_block(start):
        def take_block(weights):
            return lax.dynamic_slice_in_dim(weights, start, block_tmpl, 2).reshape(BASIS, 2 * block_tmpl)

        low_snr = contract(take_block(recon_low), series_low)
        mid_snr = contract(take_block(recon_mid), series_mid) + upsample(low_snr, kernel_table)
        full_snr = contract(take_block(recon_high), series_high) + upsample(mid_snr, kernel_table)
        return full_snr.reshape(2, block_tmpl, TIME)

    blocks = lax.map(one_block, starts)
    return jnp.transpose(blocks, (1, 0, 2, 3)).reshape(2, TEMPLATES, TIME)
```

```python
import functools
import math

import jax
import jax.numpy as jnp
import numpy as np
from jax import lax
from jax.experimental import pallas as pl
from jax.experimental.pallas import tpu as pltpu
from jax.sharding import PartitionSpec as P

RATIO = 8
HALF_TAPS = 8
LANES = 128
WIDE = 256
WINDOW = 2 * WIDE
SPAN = WINDOW // RATIO + 2 * HALF_TAPS
MESH = pl.DeviceIdType.MESH


def upsample_matrix():
    u = np.arange(SPAN)[:, None]
    v = np.arange(WINDOW)[None, :]
    lag = u - v // RATIO
    offset = (v % RATIO) / RATIO - (lag - HALF_TAPS)
    value = np.sinc(offset) * (0.5 + 0.5 * np.cos(np.pi * offset / (HALF_TAPS + 1)))
    value = np.where((lag >= 0) & (lag < 2 * HALF_TAPS), value, 0.0).astype(np.float32)
    top = value.astype(jnp.bfloat16)
    rest = (value - top.astype(np.float32)).astype(jnp.bfloat16)
    pad = np.zeros((WIDE - 3 * SPAN, WINDOW), jnp.bfloat16)
    return np.concatenate([top, top, rest, pad], axis=0)


def products(blocks):
    if blocks == 1:
        return [({0: 1}, (0,), (0,))]
    n = blocks // 2
    inner = products(n)

    def less(frames, shift):
        total = dict(frames)
        total = {m: -c for m, c in frames.items()}
        for m, c in frames.items():
            total[m + shift] = total.get(m + shift, 0) + c
        return {m: c for m, c in total.items() if c}

    both = [(f, w + tuple(i + n for i in w), o + tuple(k + n for k in o)) for f, w, o in inner]
    first = [(less(f, -n), tuple(i + n for i in w), o) for f, w, o in inner]
    last = [(less(f, n), w, tuple(k + n for k in o)) for f, w, o in inner]
    return both + first + last


def gather_kernel(
    sizes, count_ref, low_ref, mid_ref, high_ref, sl_ref, sm_ref, sh_ref, g_ref,
    recon_low, recon_mid, recon_high,
    w_out, p_out, g_out, frames_out,
    low_all, mid_all, high_all, sl_all, sm_all, sh_prev,
    low_r, mid_r, high_r, load_sem, x_full,
    fl_top, fl_rest, fm_top, fm_rest, p_full,
    strain_send, strain_recv, lz_send, lz_recv, lx_send, lx_recv,
    z_send, z_recv, x_send, x_recv, y_send, y_recv, d_send, d_recv, c_send, c_recv,
):
    bands, peers, slices, lines, parts = sizes
    rings = peers // lines
    b, p, y = lax.axis_index("band"), lax.axis_index("tmpl"), lax.axis_index("tm")
    z, x = p // lines, p % lines
    part = y % parts

    def along_z(k):
        return (b, ((z + k) % rings) * lines + x, y)

    def along_y(m):
        return (b, p, y - part + (part + m) % parts)

    across = (b, z * lines + (x + 1) % lines, y)
    sibling = (1 - b, p, y)
    before = sh_prev.shape[0]
    loads = []
    for i, (src, dst) in enumerate((
        (low_ref, low_all.at[p]), (mid_ref, mid_all.at[p]), (high_ref, high_all.at[p]),
        (sl_ref, sl_all.at[2 + y]), (sm_ref, sm_all.at[2 + y]),
        (sh_ref, x_full.at[pl.ds(before, sh_ref.shape[0])]),
        (recon_low.at[:, b, :], low_r), (recon_mid.at[:, b, :], mid_r), (recon_high.at[:, b, :], high_r),
        (g_ref, g_out),
    )):
        copy = pltpu.make_async_copy(src, dst, load_sem.at[i])
        copy.start()
        loads.append(copy)
    barrier = pltpu.get_barrier_semaphore()
    others = [along_z(k) for k in range(1, rings)] + [sibling]
    others += [(b, p, (y + k) % slices) for k in range(1, slices)]
    if lines > 1:
        others += [across]
    for device in others:
        pl.semaphore_signal(barrier, inc=1, device_id=device, device_id_type=MESH)
    pl.semaphore_wait(barrier, len(others))
    for copy in loads[:6]:
        copy.wait()

    sent, strains, landed = [], [], ([], [])

    def send(src, dst, sems, at, device):
        copy = pltpu.make_async_remote_copy(
            src_ref=src, dst_ref=dst, send_sem=sems[0].at[at], recv_sem=sems[1].at[at],
            device_id=device, device_id_type=MESH,
        )
        copy.start()
        sent.append(copy)
        return copy

    strain = (strain_send, strain_recv)
    for k in range(1, slices):
        device = (b, p, (y + k) % slices)
        strains.append(send(sl_all.at[2 + y], sl_all.at[2 + y], strain, (0, k), device))
        strains.append(send(sm_all.at[2 + y], sm_all.at[2 + y], strain, (1, k), device))
    if slices > 1:
        tail = sh_prev.shape[0]
        last = x_full.at[pl.ds(sh_ref.shape[0], tail)]
        strains.append(send(last, sh_prev, strain, (2, 1), (b, p, (y + 1) % slices)))

    arrays = ((mid_ref, mid_all), (high_ref, high_all))
    size = [ref.shape[1] // (bands * parts) for ref, _ in arrays]

    def cols(a, m=0):
        start = (b * parts + (part + m) % parts) * size[a]
        return pl.ds(pl.multiple_of(start, LANES), size[a])

    def shard(k, other=0):
        return ((z + rings - k) % rings) * lines + (x + other) % lines

    low_z = {k: send(low_all.at[p], low_all.at[p], (lz_send, lz_recv), k, along_z(k)) for k in range(1, rings)}
    from_z, from_x, from_y, from_d = {}, {}, {}, {}
    low_x = {}
    if lines > 1:
        low_x[0] = send(low_all.at[p], low_all.at[p], (lx_send, lx_recv), 0, across)
    for a, (ref, full) in enumerate(arrays):
        for k in range(1, rings):
            from_z[a, k] = send(
                full.at[p, :, cols(a)], full.at[p, :, cols(a)], (z_send, z_recv), (a, k), along_z(k)
            )
        if lines > 1:
            for m in range(parts):
                piece = send(
                    full.at[p, :, cols(a, m)], full.at[p, :, cols(a, m)],
                    (x_send, x_recv) if m == 0 else (d_send, d_recv), (a, m, 0), across,
                )
                (from_x if m == 0 else from_d)[a, m, 0] = piece
    for ref in (sl_all, sm_all):
        zero = jnp.zeros(ref.shape[1:], jnp.float32)
        for i in (0, 1, slices + 2, slices + 3):
            ref[i] = zero
    if slices == 1:
        sh_prev[...] = jnp.zeros(sh_prev.shape, jnp.float32)

    count = [0]

    def pass_on(a, view):
        at = (a, count[0])
        count[0] += 1
        landed[a].append(send(view, view, (c_send, c_recv), at, sibling))

    for copy in strains:
        copy.wait_recv()
    x_full[:before] = jnp.where(y > 0, sh_prev[...], 0.0)
    blocks = frames_out.shape[0]

    def frames_part(i):
        fill_products(x_full, frames_out, blocks * i // 3, blocks * (i + 1) // 3)

    frames_part(0)
    for k in range(1, rings):
        low_z[k].wait_recv()
        if lines > 1:
            view = low_all.at[shard(k)]
            low_x[k] = send(view, view, (lx_send, lx_recv), k, across)
    for a, (_, full) in enumerate(arrays):
        count[0] = 0
        for k in range(1, rings):
            from_z[a, k].wait_recv()
            view = full.at[shard(k), :, cols(a)]
            if lines > 1:
                from_x[a, 0, k] = send(view, view, (x_send, x_recv), (a, 0, k), across)
            for m in range(1, parts):
                from_y[a, m, k] = send(view, view, (y_send, y_recv), (a, m, k), along_y(m))
            pass_on(a, view)
    base = count[0]
    frames_part(1)
    for a, (_, full) in enumerate(arrays):
        count[0] = base
        for k in range(rings):
            if lines > 1:
                from_x[a, 0, k].wait_recv()
                view = full.at[shard(k, 1), :, cols(a)]
                if k > 0:
                    for m in range(1, parts):
                        from_d[a, m, k] = send(view, view, (d_send, d_recv), (a, m, k), along_y(m))
                pass_on(a, view)
            for m in range(1, parts):
                if k == 0:
                    continue
                from_y[a, m, k].wait_recv()
                view = full.at[shard(k), :, cols(a, parts - m)]
                pass_on(a, view)
    base = count[0]
    frames_part(2)

    def last_pieces(a, full):
        count[0] = base
        for k in range(rings):
            for m in range(1, parts):
                if lines > 1:
                    from_d[a, m, k].wait_recv()
                    shift = m if k == 0 else parts - m
                    pass_on(a, full.at[shard(k, 1), :, cols(a, shift)])

    low_here, mid_here, low_total, mid_total = bounds(sl_ref, sm_ref, slices)
    taps_low, taps_mid = low_ref.shape[1], mid_ref.shape[1]
    low_chunks, mid_chunks = (r.shape[0] // LANES - 1 for r in (fl_top, fm_top))
    rows_mid = mid_here // LANES

    def low_row(r):
        return sl_all[y + 1 - taps_low // LANES + r]

    def mid_row(r):
        at = r + (y + 2) * rows_mid - taps_mid // LANES - 1
        return sm_all[at // rows_mid, pl.ds(at % rows_mid, 1), :]

    fill_frames(shifted(low_row, HALF_TAPS + 1), fl_top, fl_rest, low_chunks)
    fill_frames(shifted(mid_row, HALF_TAPS), fm_top, fm_rest, mid_chunks)
    for copy in loads[6:]:
        copy.wait()
    last_pieces(*(0, mid_all))
    for copy in low_x.values():
        copy.wait_recv()
    low_w = split(template_filters(low_r, low_all, count_ref[2]))
    parts_low = []
    for c in range(low_chunks):
        at = (low_chunks - 1 - c) * LANES
        parts_low.append(dot3(low_w, (fl_top[at : at + LANES, :LANES], fl_rest[at : at + LANES, :LANES])))
    low = jnp.concatenate(parts_low, axis=1)
    time = y * low_here - (HALF_TAPS + 1) + lax.broadcasted_iota(jnp.int32, low.shape, 1)
    low = jnp.where((time >= 0) & (time < low_total), low, 0.0)
    for copy in landed[0]:
        copy.wait_recv()
    mid_w = split(template_filters(mid_r, mid_all, count_ref[1]))
    last_pieces(*(1, high_all))
    columns = p_full.shape[1]
    lows = [window(low, i) for i in range(-(-columns // WINDOW))]
    for start in range(0, columns, WIDE):
        size_here = min(WIDE, columns - start)
        at = (mid_chunks - taps_mid // LANES - start // LANES) * LANES
        frames = (fm_top[at : at + taps_mid, :size_here], fm_rest[at : at + taps_mid, :size_here])
        value = dot3(mid_w, frames)
        lead = start % WINDOW
        value += one_dot(lows[start // WINDOW], g_out[:, lead : lead + size_here])
        time = y * mid_here - HALF_TAPS + start + lax.broadcasted_iota(jnp.int32, value.shape, 1)
        p_full[:, start : start + size_here] = jnp.where((time >= 0) & (time < mid_total), value, 0.0)
    for i in range(p_out.shape[0]):
        base = i * (WINDOW // RATIO) // LANES * LANES
        p_out[i] = window(p_full[:, base : base + WIDE], i, base)
    for copy in landed[1]:
        copy.wait_recv()
    w = template_filters(high_r, high_all, count_ref[0])
    pieces = [w[:, i : i + WIDE] for i in range(0, w.shape[1], WIDE)]
    for i, (_, summed, _) in enumerate(products(len(pieces))):
        w_out[0, i], w_out[1, i] = split(sum(pieces[k] for k in summed))
    for copy in sent:
        copy.wait_send()


def window(value, i, base=0):
    lead = i * (WINDOW // RATIO) - base
    value = value[:, lead // LANES * LANES :][:, :WIDE]
    lead = lead % LANES
    if lead:
        value = pltpu.roll(value, WIDE - lead, 1)
    top = value.astype(jnp.bfloat16).astype(jnp.float32)
    lane = lax.broadcasted_iota(jnp.int32, value.shape, 1)
    again = jnp.where(lane < 3 * SPAN, pltpu.roll(top, 2 * SPAN, 1), 0.0)
    rest = jnp.where(lane < 2 * SPAN, pltpu.roll(value - top, SPAN, 1), again)
    return jnp.where(lane < SPAN, top, rest).astype(jnp.bfloat16)


def fill_products(x_ref, out_ref, first, last):
    lane = lax.broadcasted_iota(jnp.int32, (LANES, LANES), 1)
    lag = lax.broadcasted_iota(jnp.int32, (LANES, LANES), 0)
    per = WIDE // LANES
    steps = products(math.isqrt(4 ** int(math.log(out_ref.shape[1], 3) + 0.5)))
    blocks = len({k for _, _, outs in steps for k in outs})

    def step(s, _):
        read = {}

        def row(r):
            if r not in read:
                read[r] = x_ref[pl.ds((s + 1) * (blocks * per) + r, 1), :]
            return read[r]

        for i, (offsets, _, _) in enumerate(steps):
            def mixed(e):
                total = 0.0
                for m, c in offsets.items():
                    total = total + row(per * m + e) if c > 0 else total - row(per * m + e)
                return total

            before = staggered(mixed(-per))
            for e in range(1 - per, per):
                now = staggered(mixed(e))
                tile = split(jnp.where(lane >= lag, now, before))
                for a in range(per):
                    if 0 <= a + e < per:
                        for h in range(2):
                            out_ref[s, i, h, a * LANES : (a + 1) * LANES, (a + e) * LANES : (a + e + 1) * LANES] = tile[h]
                before = now
        return 0

    lax.fori_loop(first, last, step, 0)


def bounds(s_low, s_mid, slices):
    low, mid = s_low.shape[0] * LANES, s_mid.shape[0] * LANES
    return low, mid, low * slices, mid * slices


def template_filters(recon_ref, full, count):
    peers, rows, taps = full.shape
    first = (((0,), (0,)), ((), ()))
    index = lax.broadcasted_iota(jnp.int32, recon_ref.shape, 0)
    recon = jnp.where(index < count, recon_ref[...], 0.0)
    if rows % 8 == 0:
        return dot3(split(recon), split(full[...].reshape(peers * rows, taps)), first)
    total = 0.0
    for p in range(peers):
        total += dot3(split(recon[p * rows : (p + 1) * rows]), split(full[p]), first)
    return total


def gather(sizes, count, filters, strains, g, recons):
    low, mid, high = filters
    s_low, s_mid, s_high = strains
    bands, peers, slices = sizes
    lines = 2 if peers % 2 == 0 else 1
    rings = peers // lines
    parts = math.gcd(slices, min(mid.shape[1], high.shape[1]) // (bands * LANES))
    f32, half = jnp.float32, jnp.bfloat16
    basis, _, tmpl = recons[0].shape
    taps_low, taps_mid, taps = (f.shape[1] for f in filters)
    low_here, mid_here, _, _ = bounds(s_low, s_mid, slices)
    samples = s_high.shape[0] * LANES
    columns = mid_here + LANES
    count_products = len(products(taps // WIDE))
    vmem = pl.BlockSpec(memory_space=pltpu.VMEM)
    anywhere = pl.BlockSpec(memory_space=pltpu.HBM)
    dma = pltpu.SemaphoreType.DMA

    def two(*dims):
        return [dma(dims)] * 2

    def frames(rows):
        return [pltpu.VMEM((rows, WIDE), half)] * 2

    held = [pltpu.with_memory_space_constraint(a, pltpu.HBM) for a in (count, *filters, *strains, g, *recons)]
    return pl.pallas_call(
        functools.partial(gather_kernel, (bands, peers, slices, lines, parts)),
        out_shape=[
            pltpu.VMEM((2, count_products, tmpl, WIDE), half),
            pltpu.VMEM((samples // WINDOW, tmpl, WIDE), half),
            pltpu.VMEM(g.shape, half),
            pltpu.VMEM((samples // taps, count_products, 2, WIDE, WIDE), half),
        ],
        in_specs=[pl.BlockSpec(memory_space=pltpu.SMEM)] + [anywhere] * 10,
        out_specs=[vmem] * 4,
        scratch_shapes=[pltpu.VMEM((peers,) + a.shape, f32) for a in filters]
        + [pltpu.VMEM((slices + 4,) + a.shape, f32) for a in (s_low, s_mid)]
        + [pltpu.VMEM((taps // LANES, LANES), f32)]
        + [pltpu.VMEM((basis, tmpl), f32)] * 3
        + [dma((10,)), pltpu.VMEM(((samples + taps) // LANES, LANES), f32)]
        + frames(low_here + 2 * LANES + taps_low) + frames(columns + taps_mid)
        + [pltpu.VMEM((tmpl, columns), f32)]
        + two(3, slices) + two(rings) + two(rings) + two(2, rings)
        + two(2, parts, rings) * 3 + two(2, peers * parts),
        compiler_params=pltpu.CompilerParams(
            collective_id=0, has_side_effects=True, vmem_limit_bytes=28 * 1024 * 1024
        ),
        name="gather_filters",
    )(*held)


def split(value):
    top = value.astype(jnp.bfloat16)
    return top, (value - top.astype(jnp.float32)).astype(jnp.bfloat16)


def one_dot(u, v):
    return lax.dot_general(u, v, (((1,), (0,)), ((), ())), preferred_element_type=jnp.float32)


def dot3(a, b, dims=(((1,), (0,)), ((), ()))):
    def one(u, v):
        return lax.dot_general(u, v, dims, preferred_element_type=jnp.float32)

    return one(a[0], b[0]) + one(a[0], b[1]) + one(a[1], b[0])


def staggered(row):
    return pltpu.roll(jnp.broadcast_to(row, (LANES, LANES)), 0, 1, stride=1, stride_axis=0)


def shifted(read, by):
    lane = lax.broadcasted_iota(jnp.int32, (1, LANES), 1)

    def row(r):
        late = [pltpu.roll(read(r + i), by, 1) for i in range(2)]
        return jnp.where(lane >= by, late[1], late[0])

    return row


def fill_frames(row, top_ref, rest_ref, chunks, first=0, last=None):
    lane = lax.broadcasted_iota(jnp.int32, (LANES, LANES), 1)
    lag = lax.broadcasted_iota(jnp.int32, (LANES, LANES), 0)

    def step(c, before):
        now = staggered(row(c + 1))
        top, rest = split(jnp.where(lane >= lag, now, before))
        left = pl.multiple_of((chunks - 1 - c) * LANES, LANES)
        right = pl.multiple_of((chunks - c) * LANES, LANES)
        for ref, value in ((top_ref, top), (rest_ref, rest)):
            ref[pl.ds(left, LANES), :LANES] = value
            ref[pl.ds(right, LANES), LANES:] = value
        return now

    lax.fori_loop(first, chunks if last is None else last, step, staggered(row(first)))


def compute_kernel(strips, w_ref, p_ref, g_ref, frames_ref, out_ref, tiles, kept, sems):
    rows, count = w_ref.shape[2], w_ref.shape[1]
    depth = rows // strips
    across = tiles.shape[3] // WIDE // 2

    def write(i, q, k):
        half = i % 2
        start = pl.multiple_of((2 * i + q) * (across * WIDE) + k * WIDE, WIDE)
        at = (q * across + k) * WIDE
        return pltpu.make_async_copy(
            tiles.at[half, :, :, pl.ds(at, WIDE)], out_ref.at[:, :, pl.ds(start, WIDE)], sems.at[half, q, k]
        )

    def body(*refs):
        accs = [[refs[(q * 4 + n) * strips : (q * 4 + n + 1) * strips] for n in range(4)] for q in range(2)]

        def part(r):
            return slice(r * depth, (r + 1) * depth)

        def multiply(i, n):
            for q in range(2):
                s = 2 * i + q
                acc = accs[q][n % 4]
                ends = [e for e in (4, 5, 7, 8) if e == n]
                passes = [(frames_ref.at[s, n, 0], (w_ref.at[0, n], w_ref.at[1, n]))]
                passes += [(frames_ref.at[s, n, 1], (w_ref.at[0, n],))]
                if ends:
                    k = ends_at[n]
                    lead = k * WIDE % WINDOW
                    passes += [(g_ref.at[:, lead : lead + WIDE], (p_ref.at[s * (across * WIDE // WINDOW) + k * WIDE // WINDOW],))]
                for step, (right, lefts) in enumerate(passes):
                    staged = (n + step) % 2
                    pltpu.matmul_push_rhs(right[...], staged, q)
                    for turn, left in enumerate(lefts):
                        for r in range(strips):
                            first = staged if turn == 0 and r == 0 else None
                            pltpu.matmul_acc_lhs(acc[r], left[part(r), :], first)

        ends_at = {4: 0, 5: 1, 7: 2, 8: 3}

        def finish(i, n):
            half = i % 2
            for q in range(2):
                for r in range(strips):
                    value = pltpu.matmul_pop(accs[q][n % 4][r])
                    at = (q, slice(None), part(r))
                    if n == 0:
                        kept[q, 0, part(r)] = value
                    elif n in (1, 2):
                        kept[q, n, part(r)] = kept[q, 0, part(r)] + value
                    elif n in (3, 6):
                        kept[q, 3, part(r)] = kept[q, 1, part(r)] + value
                        kept[q, 4, part(r)] = kept[q, 2, part(r)] + value
                    else:
                        k = ends_at[n]
                        at = (q * across + k) * WIDE
                        tiles[half, 0, part(r), at : at + WIDE] = kept[q, 3 + (n - 1) % 3, part(r)] + value
                if n in ends_at:
                    write(i, q, ends_at[n]).start()

        def step(i, _):
            @pl.when(i > 1)
            def _():
                for q in range(2):
                    for k in range(across):
                        write(i - 2, q, k).wait()

            for n in range(count):
                multiply(i, n)
                if n > 0:
                    finish(i, n - 1)
            finish(i, count - 1)
            return 0

        trips = frames_ref.shape[0] // 2
        lax.fori_loop(0, trips, step, 0)
        for i in range(max(0, trips - 2), trips):
            for q in range(2):
                for k in range(across):
                    write(i, q, k).wait()

    specs = []
    for q in range(2):
        specs += [pltpu.ACC(q)((depth, WIDE), jnp.float32)] * (4 * strips)
    pl.run_scoped(body, *specs)


def compute(w, p, g, frames):
    tmpl = w.shape[2]
    blocks = len({k for _, _, outs in products(4) for k in outs})
    samples = frames.shape[0] * blocks * WIDE
    vmem = pl.BlockSpec(memory_space=pltpu.VMEM)
    return pl.pallas_call(
        functools.partial(compute_kernel, max(1, tmpl // 64)),
        out_shape=jax.ShapeDtypeStruct((1, tmpl, samples), jnp.float32),
        in_specs=[vmem] * 4,
        out_specs=pl.BlockSpec(memory_space=pltpu.HBM),
        scratch_shapes=[
            pltpu.VMEM((2, 1, tmpl, 2 * blocks * WIDE), jnp.float32),
            pltpu.VMEM((2, 5, tmpl, WIDE), jnp.float32),
            pltpu.SemaphoreType.DMA((2, 2, blocks)),
        ],
        compiler_params=pltpu.CompilerParams(vmem_limit_bytes=12 * 1024 * 1024),
        name="filter_templates",
    )(w, p, g, frames)


def local(
    sizes, strain_high, strain_mid, strain_low, filters_high, filters_mid, filters_low,
    recon_high, recon_mid, recon_low, basis_count,
):
    g = jnp.asarray(upsample_matrix())
    strains = [s.reshape(-1, LANES) for s in (strain_low, strain_mid, strain_high)]
    out = gather(
        sizes, basis_count, (filters_low, filters_mid, filters_high), strains, g,
        (recon_low, recon_mid, recon_high),
    )
    return compute(*out)


def solution(mesh):
    sizes = tuple(mesh.shape[name] for name in ("band", "tmpl", "tm"))
    in_specs = (
        P("tm"), P("tm"), P("tm"),
        P("tmpl", None), P("tmpl", None), P("tmpl", None),
        P(None, None, "tmpl"), P(None, None, "tmpl"), P(None, None, "tmpl"),
        P(),
    )
    return jax.shard_map(
        functools.partial(local, sizes), mesh=mesh, in_specs=in_specs,
        out_specs=P("band", "tmpl", "tm"), check_vma=False,
    )
```

```python
import functools
import math

import jax
import jax.numpy as jnp
import numpy as np
from jax import lax
from jax.experimental import pallas as pl
from jax.experimental.pallas import tpu as pltpu
from jax.sharding import PartitionSpec as P

RATIO = 8
HALF_TAPS = 8
LANES = 128
WIDE = 256
WINDOW = 2 * WIDE
SPAN = WINDOW // RATIO + 2 * HALF_TAPS
MESH = pl.DeviceIdType.MESH


def upsample_matrix():
    u = np.arange(SPAN)[:, None]
    v = np.arange(WINDOW)[None, :]
    lag = u - v // RATIO
    offset = (v % RATIO) / RATIO - (lag - HALF_TAPS)
    value = np.sinc(offset) * (0.5 + 0.5 * np.cos(np.pi * offset / (HALF_TAPS + 1)))
    value = np.where((lag >= 0) & (lag < 2 * HALF_TAPS), value, 0.0).astype(np.float32)
    top = value.astype(jnp.bfloat16)
    rest = (value - top.astype(np.float32)).astype(jnp.bfloat16)
    pad = np.zeros((WIDE - 3 * SPAN, WINDOW), jnp.bfloat16)
    return np.concatenate([top, top, rest, pad], axis=0)


def products(blocks):
    if blocks == 1:
        return [({0: 1}, (0,), (0,))]
    n = blocks // 2
    inner = products(n)

    def less(frames, shift):
        total = dict(frames)
        total = {m: -c for m, c in frames.items()}
        for m, c in frames.items():
            total[m + shift] = total.get(m + shift, 0) + c
        return {m: c for m, c in total.items() if c}

    both = [(f, w + tuple(i + n for i in w), o + tuple(k + n for k in o)) for f, w, o in inner]
    first = [(less(f, -n), tuple(i + n for i in w), o) for f, w, o in inner]
    last = [(less(f, n), w, tuple(k + n for k in o)) for f, w, o in inner]
    return both + first + last


def gather_kernel(
    sizes, count_ref, low_ref, mid_ref, high_ref, sl_ref, sm_ref, sh_ref, g_ref,
    recon_low, recon_mid, recon_high,
    w_out, p_full, g_out, frames_out,
    low_all, mid_all, high_all, sl_all, sm_all, sh_prev,
    low_r, mid_r, high_r, low_l, mid_l, high_l, load_sem, x_full,
    fl_top, fl_rest, fm_top, fm_rest, wm_top, wm_rest, lows, w_full,
    strain_send, strain_recv, lo_send, lf_send, lz_recv, lx_send, lx_recv, lc_send, lc_recv,
    zo_send, zf_send, z_recv, x_send, x_recv, y_send, y_recv, d_send, d_recv, c_send, c_recv,
):
    bands, peers, slices, lines, parts = sizes
    rings = peers // lines
    b, p, y = lax.axis_index("band"), lax.axis_index("tmpl"), lax.axis_index("tm")
    z, x = p // lines, p % lines
    part = y % parts

    def at_level(level):
        return (b, ((level + rings) % rings) * lines + x, y)

    def on_line(level):
        return (level >= 0) & (level < rings)

    def along_y(m):
        return (b, p, y - part + (part + m) % parts)

    across = (b, z * lines + (x + 1) % lines, y)
    sibling = (1 - b, p, y)
    before = sh_prev.shape[0]
    loads = []
    for i, (src, dst) in enumerate((
        (low_ref, low_all.at[p]), (mid_ref, mid_all.at[p]), (high_ref, high_all.at[p]),
        (sl_ref, sl_all.at[2 + y]), (sm_ref, sm_all.at[2 + y]),
        (sh_ref, x_full.at[pl.ds(before, sh_ref.shape[0])]),
        (recon_low.at[:, b, :], low_r), (recon_mid.at[:, b, :], mid_r), (recon_high.at[:, b, :], high_r),
        (g_ref, g_out),
    )):
        copy = pltpu.make_async_copy(src, dst, load_sem.at[i])
        copy.start()
        loads.append(copy)

    reach = [1, -1] if rings > 1 else []
    barrier = pltpu.get_barrier_semaphore()

    def greet(device):
        pl.semaphore_signal(barrier, inc=1, device_id=device, device_id_type=MESH)

    others = [sibling] + [(b, p, (y + k) % slices) for k in range(1, slices)]
    if lines > 1:
        others += [across]
    for device in others:
        greet(device)
    waiting = len(others)
    for step in reach:
        pl.when(on_line(z + step))(functools.partial(greet, at_level(z + step)))
        waiting = waiting + jnp.where(on_line(z + step), 1, 0)
    pl.semaphore_wait(barrier, waiting)
    for copy in loads[:6]:
        copy.wait()

    sent = []

    def remote(view, out, into, device):
        return pltpu.make_async_remote_copy(
            src_ref=view, dst_ref=view, send_sem=out, recv_sem=into, device_id=device, device_id_type=MESH
        )

    def send(view, out, into, device, when=None):
        copy = remote(view, out, into, device)
        if when is None:
            copy.start()
        else:
            pl.when(when)(copy.start)
        sent.append((copy, when))

    def arrived(view, out, into, when=None):
        copy = remote(view, out, into, sibling)
        if when is None:
            copy.wait_recv()
        else:
            pl.when(when)(copy.wait_recv)

    near = jnp.minimum(z, rings - 1 - z)
    longer = jnp.where(z < rings - 1 - z, 1, -1)
    levels = [(z, 0)]
    for n in range(1, rings):
        inside = n <= 2 * near
        step = jnp.where(inside, 1 - 2 * (n % 2), longer)
        d = jnp.where(inside, (n + 1) // 2, n - near)
        levels.append((z + step * d, step))

    arrays = (mid_all, high_all)
    size = [ref.shape[2] // (bands * parts) for ref in arrays]

    def cols(a, m=0, band=b):
        start = (band * parts + (part + m) % parts) * size[a]
        return pl.ds(pl.multiple_of(start, LANES), size[a])

    def piece(a, n, other=0, m=0, band=b):
        return arrays[a].at[levels[n][0] * lines + (x + other) % lines, :, cols(a, m, band)]

    mine = x % bands == b

    def low(n, other=0):
        return low_all.at[levels[n][0] * lines + (x + other) % lines]

    def own_low():
        for i, step in enumerate(reach):
            send(low(0), lo_send.at[i], lz_recv.at[z], at_level(z + step), mine & on_line(z + step))
        if lines > 1:
            send(low(0), lx_send.at[z], lx_recv.at[z], across, mine)

    def own_z(a):
        for i, step in enumerate(reach):
            send(piece(a, 0), zo_send.at[a, i], z_recv.at[a, z], at_level(z + step), on_line(z + step))

    def own_x(a, m):
        if lines > 1:
            send(piece(a, 0, 0, m), x_send.at[a, m, z], x_recv.at[a, m, z], across)

    def low_from_z(n):
        level, step = levels[n]
        ahead = z - step
        arrived(low(n), lf_send.at[level], lz_recv.at[level], mine)
        send(low(n), lf_send.at[level], lz_recv.at[level], at_level(ahead), mine & on_line(ahead))
        if lines > 1:
            send(low(n), lx_send.at[level], lx_recv.at[level], across, mine)
        send(low(n), lc_send.at[0, level], lc_recv.at[0, level], sibling, mine)

    def low_from_x(n):
        if lines > 1:
            level = levels[n][0]
            arrived(low(n, 1), lx_send.at[level], lx_recv.at[level], jnp.logical_not(mine))
            send(low(n, 1), lc_send.at[1, level], lc_recv.at[1, level], sibling, jnp.logical_not(mine))

    def low_landed():
        for n in range(rings):
            level = levels[n][0]
            if n > 0:
                arrived(low(n), lc_send.at[0, level], lc_recv.at[0, level], jnp.logical_not(mine))
            if lines > 1:
                arrived(low(n, 1), lc_send.at[1, level], lc_recv.at[1, level], mine)

    def pass_on(a, line, n, m, view):
        level = levels[n][0]
        send(view, c_send.at[a, line, m, level], c_recv.at[a, line, m, level], sibling)

    def from_z(a, n):
        level, step = levels[n]
        ahead = z - step
        view = piece(a, n)
        arrived(view, zf_send.at[a, level], z_recv.at[a, level])
        send(view, zf_send.at[a, level], z_recv.at[a, level], at_level(ahead), on_line(ahead))
        if lines > 1:
            send(view, x_send.at[a, 0, level], x_recv.at[a, 0, level], across)
        for m in range(1, parts):
            send(view, y_send.at[a, m, level], y_recv.at[a, m, level], along_y(m))
        pass_on(a, 0, n, 0, view)

    def from_x(a, n, m=0):
        if lines > 1:
            level = levels[n][0]
            view = piece(a, n, 1, m)
            arrived(view, x_send.at[a, m, level], x_recv.at[a, m, level])
            if n > 0:
                for k in range(1, parts):
                    send(view, d_send.at[a, k, level], d_recv.at[a, k, level], along_y(k))
            pass_on(a, 1, n, m, view)

    def from_y(a, n):
        level = levels[n][0]
        for m in range(1, parts):
            view = piece(a, n, 0, parts - m)
            arrived(view, y_send.at[a, m, level], y_recv.at[a, m, level])
            pass_on(a, 0, n, m, view)

    def from_xy(a, n):
        if lines > 1:
            level = levels[n][0]
            for m in range(1, parts):
                view = piece(a, n, 1, parts - m)
                arrived(view, d_send.at[a, m, level], d_recv.at[a, m, level])
                pass_on(a, 1, n, m, view)

    def landed(a, own):
        for n in range(rings):
            level = levels[n][0]
            for m in range(1) if own else range(1, parts):
                if n > 0:
                    view = piece(a, n, 0, (parts - m) % parts, 1 - b)
                    arrived(view, c_send.at[a, 0, m, level], c_recv.at[a, 0, m, level])
                if lines > 1:
                    view = piece(a, n, 1, m if n == 0 else (parts - m) % parts, 1 - b)
                    arrived(view, c_send.at[a, 1, m, level], c_recv.at[a, 1, m, level])

    def blocks(a, own):
        parted = range(1) if own else range(1, parts)
        return [(cols(a, m, band), (band * parts + (part + m) % parts) * size[a]) for m in parted for band in range(bands)]

    strains = []
    for k in range(1, slices):
        device = (b, p, (y + k) % slices)
        for i, ref in enumerate((sl_all, sm_all)):
            send(ref.at[2 + y], strain_send.at[i, k], strain_recv.at[i, k], device)
            strains.append((ref.at[2 + (y + slices - k) % slices], strain_send.at[i, k], strain_recv.at[i, k]))
    if slices > 1:
        tail = pl.ds(x_full.shape[0] - before, before)
        copy = pltpu.make_async_remote_copy(
            src_ref=x_full.at[tail], dst_ref=sh_prev, send_sem=strain_send.at[2, 0], recv_sem=strain_recv.at[2, 0],
            device_id=(b, p, (y + 1) % slices), device_id_type=MESH,
        )
        copy.start()
        sent.append((copy, None))

    own_low()
    for a in range(2):
        own_z(a)
        own_x(a, 0)
    for a in range(2):
        for m in range(1, parts):
            own_x(a, m)

    low_here, mid_here, low_total, mid_total = bounds(sl_ref, sm_ref, slices)
    taps_low, taps_mid = low_ref.shape[1], mid_ref.shape[1]
    low_chunks, mid_chunks = (r.shape[0] // LANES - 1 for r in (fl_top, fm_top))
    rows_mid = mid_here // LANES
    columns = p_full.shape[1]

    def low_row(r):
        return sl_all[y + 1 - taps_low // LANES + r]

    def mid_row(r):
        at = r + (y + 2) * rows_mid - taps_mid // LANES - 1
        return sm_all[at // rows_mid, pl.ds(at % rows_mid, 1), :]

    recons = ((low_r, low_l), (mid_r, mid_l), (high_r, high_l))

    def prepare(i):
        loads[6 + i].wait()
        spread_recon(*recons[i], count_ref[2 - i])

    work = [functools.partial(fill_frames, shifted(low_row, HALF_TAPS + 1), fl_top, fl_rest, low_chunks, 0, low_chunks)]
    for first in range(0, mid_chunks, 3):
        last = min(mid_chunks, first + 3)
        work += [functools.partial(fill_frames, shifted(mid_row, HALF_TAPS), fm_top, fm_rest, mid_chunks, first, last)]
    total = frames_out.shape[1]
    for block in range(frames_out.shape[0]):
        for first, last in ((0, total // 2 + 1), (total // 2 + 1, total)):
            work += [functools.partial(fill_products, x_full, frames_out, block, first, last)]

    def spend(count):
        for _ in range(count):
            if work:
                work.pop(0)()

    others = range(1, rings)
    prepare(0)
    prepare(1)
    prepare(2)
    loads[9].wait()
    for ref in (sl_all, sm_all):
        zero = jnp.zeros(ref.shape[1:], jnp.float32)
        for i in (0, 1, slices + 2, slices + 3):
            ref[i] = zero
    if slices == 1:
        sh_prev[...] = jnp.zeros(sh_prev.shape, jnp.float32)
    else:
        copy.wait_recv()
    for view in strains:
        arrived(*view)
    x_full[:before] = jnp.where(y > 0, sh_prev[...], 0.0)
    spend(1)
    starts = range(0, columns, WIDE)

    def mid_tile(start, own):
        size_here = min(WIDE, columns - start)
        at = (mid_chunks - taps_mid // LANES - start // LANES) * LANES
        tile = slice(start, start + size_here)
        value = 0.0 if own else p_full[:, tile]
        for lanes, first in blocks(0, own):
            rows = pl.ds(pl.multiple_of(at + first, LANES), size[0])
            value += dot3((wm_top[:, lanes], wm_rest[:, lanes]), (fm_top[rows, :size_here], fm_rest[rows, :size_here]))
        if own:
            lead = start % WINDOW
            value += one_dot(lows[start // WINDOW], g_out[:, lead : lead + size_here])
        else:
            time = y * mid_here - HALF_TAPS + start + lax.broadcasted_iota(jnp.int32, value.shape, 1)
            value = jnp.where((time >= 0) & (time < mid_total), value, 0.0)
        p_full[:, tile] = value

    def mid_filters(own):
        for lanes, _ in blocks(0, own):
            wm_top[:, lanes], wm_rest[:, lanes] = split(template_filters(mid_r, mid_l, mid_all, lanes, count_ref[1]))

    def high_filters(own):
        for lanes, _ in blocks(1, own):
            w_full[:, lanes] = template_filters(high_r, high_l, high_all, lanes, count_ref[0])

    def low_part():
        low_w = split(template_filters(low_r, low_l, low_all, slice(None), count_ref[2]))
        parts_low = []
        for c in range(low_chunks):
            at = (low_chunks - 1 - c) * LANES
            parts_low.append(dot3(low_w, (fl_top[at : at + LANES, :LANES], fl_rest[at : at + LANES, :LANES])))
        value = jnp.concatenate(parts_low, axis=1)
        time = y * low_here - (HALF_TAPS + 1) + lax.broadcasted_iota(jnp.int32, value.shape, 1)
        value = jnp.where((time >= 0) & (time < low_total), value, 0.0)
        for i in range(lows.shape[0]):
            lows[i] = window(value, i * (WINDOW // RATIO))

    for a in range(2):
        for n in others[:2]:
            from_z(a, n)
    for n in others[:2]:
        low_from_z(n)
    spend(3)
    for n in others[2:]:
        from_z(0, n)
        low_from_z(n)
        from_z(1, n)
    spend(1)
    for n in others[:2]:
        from_x(0, n)
    spend(1)
    for n in range(rings):
        low_from_x(n)
    from_x(0, 0)
    spend(1)
    for n in others[2:]:
        from_x(0, n)
    for m in range(1, parts):
        from_x(0, 0, m)
    spend(1)
    low_landed()
    low_part()
    for n in others[:2]:
        from_x(1, n)
    landed(0, True)
    mid_filters(True)
    for n in others[:2]:
        from_y(0, n)
    steps = [functools.partial(from_x, 1, n) for n in others[2:]]
    steps += [functools.partial(from_y, 0, n) for n in others[2:]]
    steps += [functools.partial(from_xy, 0, n) for n in others]
    steps += [functools.partial(from_x, 1, 0)]
    for start in starts:
        mid_tile(start, True)
        if steps:
            steps.pop(0)()
        spend(1)
    for step in steps:
        step()
        spend(1)
    for n in others:
        from_y(1, n)
    spend(3)
    for m in range(1, parts):
        from_x(1, 0, m)
    landed(1, True)
    high_filters(True)
    spend(2)
    landed(0, False)
    mid_filters(False)
    later = list(others)
    for start in starts:
        mid_tile(start, False)
        if later:
            from_xy(1, later.pop(0))
    for n in later:
        from_xy(1, n)
    spend(len(work))
    landed(1, False)
    high_filters(False)
    pieces = [w_full[:, i : i + WIDE] for i in range(0, w_full.shape[1], WIDE)]
    for i, (_, summed, _) in enumerate(products(len(pieces))):
        w_out[0, i], w_out[1, i] = split(sum(pieces[k] for k in summed))
    for copy, when in sent:
        if when is None:
            copy.wait_send()
        else:
            pl.when(when)(copy.wait_send)


def spread_recon(recon_ref, out_ref, count):
    index = lax.broadcasted_iota(jnp.int32, recon_ref.shape, 0)
    top, rest = split(jnp.where(index < count, recon_ref[...], 0.0).T)
    out_ref[...] = jnp.concatenate([top, rest, top], axis=1)


def window(value, lead):
    value = value[:, lead // LANES * LANES :][:, :WIDE]
    lead = lead % LANES
    if lead:
        value = pltpu.roll(value, WIDE - lead, 1)
    top = value.astype(jnp.bfloat16).astype(jnp.float32)
    lane = lax.broadcasted_iota(jnp.int32, value.shape, 1)
    again = jnp.where(lane < 3 * SPAN, pltpu.roll(top, 2 * SPAN, 1), 0.0)
    rest = jnp.where(lane < 2 * SPAN, pltpu.roll(value - top, SPAN, 1), again)
    return jnp.where(lane < SPAN, top, rest).astype(jnp.bfloat16)


def fill_products(x_ref, out_ref, block, first, last):
    lane = lax.broadcasted_iota(jnp.int32, (LANES, LANES), 1)
    lag = lax.broadcasted_iota(jnp.int32, (LANES, LANES), 0)
    per = WIDE // LANES
    steps = products(2 ** round(math.log(out_ref.shape[1], 3)))
    start = (block + 1) * per * len({k for _, _, outs in steps for k in outs})
    for i, (offsets, _, _) in list(enumerate(steps))[first:last]:
        before = None
        for e in range(-per, per):
            mixed = 0.0
            for m, c in offsets.items():
                row = x_ref[start + per * m + e : start + per * m + e + 1, :]
                mixed = mixed + row if c > 0 else mixed - row
            now = staggered(mixed)
            if before is not None:
                tile = split(jnp.where(lane >= lag, now, before))
                for a in range(max(0, -e), min(per, per - e)):
                    for h in range(2):
                        out_ref[block, i, h, a * LANES : (a + 1) * LANES, (a + e) * LANES : (a + e + 1) * LANES] = tile[h]
            before = now


def bounds(s_low, s_mid, slices):
    low, mid = s_low.shape[0] * LANES, s_mid.shape[0] * LANES
    return low, mid, low * slices, mid * slices


def template_filters(recon_ref, spread_ref, full, lanes, count):
    peers, rows, _ = full.shape
    if rows % 8 == 0:
        filters = full[:, :, lanes]
        top, rest = split(filters.reshape(peers * rows, filters.shape[2]))
        return one_dot(spread_ref[...], jnp.concatenate([top, top, rest], axis=0))
    first = (((0,), (0,)), ((), ()))
    index = lax.broadcasted_iota(jnp.int32, recon_ref.shape, 0)
    recon = jnp.where(index < count, recon_ref[...], 0.0)
    total = 0.0
    for p in range(peers):
        total += dot3(split(recon[p * rows : (p + 1) * rows]), split(full[p, :, lanes]), first)
    return total


def gather(sizes, count, filters, strains, g, recons):
    low, mid, high = filters
    s_low, s_mid, s_high = strains
    bands, peers, slices = sizes
    lines = 2 if peers % 2 == 0 else 1
    rings = peers // lines
    parts = math.gcd(slices, min(mid.shape[1], high.shape[1]) // (bands * LANES))
    f32, half = jnp.float32, jnp.bfloat16
    basis, _, tmpl = recons[0].shape
    taps_low, taps_mid, taps = (f.shape[1] for f in filters)
    low_here, mid_here, _, _ = bounds(s_low, s_mid, slices)
    samples = s_high.shape[0] * LANES
    columns = mid_here + LANES
    count_products = len(products(taps // WIDE))
    vmem = pl.BlockSpec(memory_space=pltpu.VMEM)
    anywhere = pl.BlockSpec(memory_space=pltpu.HBM)
    dma = pltpu.SemaphoreType.DMA

    def two(*dims):
        return [dma(dims)] * 2

    def frames(rows):
        return [pltpu.VMEM((rows, WIDE), half)] * 2

    held = [pltpu.with_memory_space_constraint(a, pltpu.HBM) for a in (count, *filters, *strains, g, *recons)]
    return pl.pallas_call(
        functools.partial(gather_kernel, (bands, peers, slices, lines, parts)),
        out_shape=[
            pltpu.VMEM((2, count_products, tmpl, WIDE), half),
            pltpu.VMEM((tmpl, columns), f32),
            pltpu.VMEM(g.shape, half),
            pltpu.VMEM((samples // taps, count_products, 2, WIDE, WIDE), half),
        ],
        in_specs=[pl.BlockSpec(memory_space=pltpu.SMEM)] + [anywhere] * 10,
        out_specs=[vmem] * 4,
        scratch_shapes=[pltpu.VMEM((peers,) + a.shape, f32) for a in filters]
        + [pltpu.VMEM((slices + 4,) + a.shape, f32) for a in (s_low, s_mid)]
        + [pltpu.VMEM((taps // LANES, LANES), f32)]
        + [pltpu.VMEM((basis, tmpl), f32)] * 3 + [pltpu.VMEM((tmpl, 3 * basis), half)] * 3
        + [dma((10,)), pltpu.VMEM(((samples + taps) // LANES, LANES), f32)]
        + frames(low_here + 2 * LANES + taps_low) + frames(columns + taps_mid)
        + [pltpu.VMEM((tmpl, taps_mid), half)] * 2
        + [pltpu.VMEM((-(-columns // WINDOW), tmpl, WIDE), half), pltpu.VMEM((tmpl, taps), f32)]
        + two(3, slices) + [dma((2,)), dma((rings,)), dma((rings,))] + two(rings) + two(2, rings)
        + [dma((2, 2)), dma((2, rings)), dma((2, rings))]
        + two(2, parts, rings) * 3 + two(2, 2, parts, rings),
        compiler_params=pltpu.CompilerParams(
            collective_id=0, has_side_effects=True, vmem_limit_bytes=28 * 1024 * 1024
        ),
        name="gather_filters",
    )(*held)


def split(value):
    top = value.astype(jnp.bfloat16)
    return top, (value - top.astype(jnp.float32)).astype(jnp.bfloat16)


def one_dot(u, v):
    return lax.dot_general(u, v, (((1,), (0,)), ((), ())), preferred_element_type=jnp.float32)


def dot3(a, b, dims=(((1,), (0,)), ((), ()))):
    def one(u, v):
        return lax.dot_general(u, v, dims, preferred_element_type=jnp.float32)

    return one(a[0], b[0]) + one(a[0], b[1]) + one(a[1], b[0])


def staggered(row):
    return pltpu.roll(jnp.broadcast_to(row, (LANES, LANES)), 0, 1, stride=1, stride_axis=0)


def shifted(read, by):
    lane = lax.broadcasted_iota(jnp.int32, (1, LANES), 1)

    def row(r):
        late = [pltpu.roll(read(r + i), by, 1) for i in range(2)]
        return jnp.where(lane >= by, late[1], late[0])

    return row


def fill_frames(row, top_ref, rest_ref, chunks, first, last):
    lane = lax.broadcasted_iota(jnp.int32, (LANES, LANES), 1)
    lag = lax.broadcasted_iota(jnp.int32, (LANES, LANES), 0)
    before = staggered(row(first))
    for c in range(first, last):
        now = staggered(row(c + 1))
        top, rest = split(jnp.where(lane >= lag, now, before))
        left, right = (chunks - 1 - c) * LANES, (chunks - c) * LANES
        for ref, value in ((top_ref, top), (rest_ref, rest)):
            ref[left : left + LANES, :LANES] = value
            ref[right : right + LANES, LANES:] = value
        before = now


def compute_kernel(strips, w_ref, p_ref, g_ref, frames_ref, out_ref, tiles, kept, spread, sems):
    rows, count = w_ref.shape[2], w_ref.shape[1]
    depth = rows // strips
    across = tiles.shape[3] // WIDE // 2

    def write(i, q, k):
        half = i % 2
        start = pl.multiple_of((2 * i + q) * (across * WIDE) + k * WIDE, WIDE)
        at = (q * across + k) * WIDE
        return pltpu.make_async_copy(
            tiles.at[half, :, :, pl.ds(at, WIDE)], out_ref.at[:, :, pl.ds(start, WIDE)], sems.at[half, q, k]
        )

    def body(*refs):
        accs = [[refs[(q * 4 + n) * strips : (q * 4 + n + 1) * strips] for n in range(4)] for q in range(2)]

        def part(r):
            return slice(r * depth, (r + 1) * depth)

        def multiply(i, n):
            for q in range(2):
                s = 2 * i + q
                acc = accs[q][n % 4]
                ends = [e for e in (4, 5, 7, 8) if e == n]
                passes = [(frames_ref.at[s, n, 0], (w_ref.at[0, n], w_ref.at[1, n]))]
                passes += [(frames_ref.at[s, n, 1], (w_ref.at[0, n],))]
                if ends:
                    k = ends_at[n]
                    lead = k * WIDE % WINDOW
                    passes += [(g_ref.at[:, lead : lead + WIDE], (spread.at[(q * across + k) * WIDE // WINDOW],))]
                for step, (right, lefts) in enumerate(passes):
                    staged = (n + step) % 2
                    pltpu.matmul_push_rhs(right[...], staged, q)
                    for turn, left in enumerate(lefts):
                        for r in range(strips):
                            first = staged if turn == 0 and r == 0 else None
                            pltpu.matmul_acc_lhs(acc[r], left[part(r), :], first)

        ends_at = {4: 0, 5: 1, 7: 2, 8: 3}

        def finish(i, n):
            half = i % 2
            for q in range(2):
                for r in range(strips):
                    value = pltpu.matmul_pop(accs[q][n % 4][r])
                    at = (q, slice(None), part(r))
                    if n == 0:
                        kept[q, 0, part(r)] = value
                    elif n in (1, 2):
                        kept[q, n, part(r)] = kept[q, 0, part(r)] + value
                    elif n in (3, 6):
                        kept[q, 3, part(r)] = kept[q, 1, part(r)] + value
                        kept[q, 4, part(r)] = kept[q, 2, part(r)] + value
                    else:
                        k = ends_at[n]
                        at = (q * across + k) * WIDE
                        tiles[half, 0, part(r), at : at + WIDE] = kept[q, 3 + (n - 1) % 3, part(r)] + value
                if n in ends_at:
                    write(i, q, ends_at[n]).start()

        def step(i, _):
            @pl.when(i > 1)
            def _():
                for q in range(2):
                    for k in range(across):
                        write(i - 2, q, k).wait()

            stride = WINDOW // RATIO
            span = spread.shape[0] * stride
            for j in range(spread.shape[0]):
                lead = j * stride % LANES
                base = pl.multiple_of(i * span + j * stride // LANES * LANES, LANES)
                for r in range(strips):
                    spread[j, part(r)] = window(p_ref[part(r), pl.ds(base, WIDE)], lead)
            for n in range(count):
                multiply(i, n)
                if n > 0:
                    finish(i, n - 1)
            finish(i, count - 1)
            return 0

        trips = frames_ref.shape[0] // 2
        lax.fori_loop(0, trips, step, 0)
        for i in range(max(0, trips - 2), trips):
            for q in range(2):
                for k in range(across):
                    write(i, q, k).wait()

    specs = []
    for q in range(2):
        specs += [pltpu.ACC(q)((depth, WIDE), jnp.float32)] * (4 * strips)
    pl.run_scoped(body, *specs)


def compute(w, p, g, frames):
    tmpl = w.shape[2]
    blocks = len({k for _, _, outs in products(4) for k in outs})
    samples = frames.shape[0] * blocks * WIDE
    vmem = pl.BlockSpec(memory_space=pltpu.VMEM)
    return pl.pallas_call(
        functools.partial(compute_kernel, max(1, tmpl // 64)),
        out_shape=jax.ShapeDtypeStruct((1, tmpl, samples), jnp.float32),
        in_specs=[vmem] * 4,
        out_specs=pl.BlockSpec(memory_space=pltpu.HBM),
        scratch_shapes=[
            pltpu.VMEM((2, 1, tmpl, 2 * blocks * WIDE), jnp.float32),
            pltpu.VMEM((2, 5, tmpl, WIDE), jnp.float32),
            pltpu.VMEM((2 * blocks * WIDE // WINDOW, tmpl, WIDE), jnp.bfloat16),
            pltpu.SemaphoreType.DMA((2, 2, blocks)),
        ],
        compiler_params=pltpu.CompilerParams(vmem_limit_bytes=12 * 1024 * 1024),
        name="filter_templates",
    )(w, p, g, frames)


def local(
    sizes, strain_high, strain_mid, strain_low, filters_high, filters_mid, filters_low,
    recon_high, recon_mid, recon_low, basis_count,
):
    g = jnp.asarray(upsample_matrix())
    strains = [s.reshape(-1, LANES) for s in (strain_low, strain_mid, strain_high)]
    out = gather(
        sizes, basis_count, (filters_low, filters_mid, filters_high), strains, g,
        (recon_low, recon_mid, recon_high),
    )
    return compute(*out)


def solution(mesh):
    sizes = tuple(mesh.shape[name] for name in ("band", "tmpl", "tm"))
    in_specs = (
        P("tm"), P("tm"), P("tm"),
        P("tmpl", None), P("tmpl", None), P("tmpl", None),
        P(None, None, "tmpl"), P(None, None, "tmpl"), P(None, None, "tmpl"),
        P(),
    )
    return jax.shard_map(
        functools.partial(local, sizes), mesh=mesh, in_specs=in_specs,
        out_specs=P("band", "tmpl", "tm"), check_vma=False,
    )
```

```python
import functools
import math

import jax
import jax.numpy as jnp
import numpy as np
from jax import lax
from jax.experimental import pallas as pl
from jax.experimental.pallas import tpu as pltpu
from jax.sharding import PartitionSpec as P

RATIO = 8
HALF_TAPS = 8
LANES = 128
WIDE = 256
WINDOW = 2 * WIDE
SPAN = WINDOW // RATIO + 2 * HALF_TAPS
MESH = pl.DeviceIdType.MESH
ORDER = (
    ("f", 2), ("z", 0, 1), ("z", 0, 2), ("f", 2), ("x", 0, 0), ("f", 1), ("z", 1, 1), ("z", 1, 2), ("f", 5),
    ("b", 1, 0), ("z", 0, 3), ("f", 1), ("y", 0, 1), ("f", 1), ("x", 0, 1), ("f", 1), ("z", 1, 3), ("f", 1),
    ("y", 0, 2), ("y", 1, 1), ("x", 0, 2), ("x", 1, 0), ("f", 1), ("b", 0, 0), ("x", 1, 1), ("f", 1), ("y", 1, 2),
    ("f", 1), ("x", 0, 3), ("l",), ("y", 0, 3), ("f", 2), ("x", 1, 3), ("d", 0, 1), ("m", 1), ("x", 1, 2), ("t", 1),
    ("t", 1), ("d", 0, 2), ("f", 2), ("y", 1, 3), ("d", 0, 3), ("f", 1), ("t", 1), ("t", 1), ("d", 1, 1), ("t", 1),
    ("d", 1, 3), ("m", 0), ("t", 0), ("t", 0), ("d", 1, 2), ("t", 0), ("t", 0), ("h", 1), ("t", 0), ("f", 1),
)
LATE_X = ((0, 2), (1, 1))


def upsample_matrix():
    u = np.arange(SPAN)[:, None]
    v = np.arange(WINDOW)[None, :]
    lag = u - v // RATIO
    offset = (v % RATIO) / RATIO - (lag - HALF_TAPS)
    value = np.sinc(offset) * (0.5 + 0.5 * np.cos(np.pi * offset / (HALF_TAPS + 1)))
    value = np.where((lag >= 0) & (lag < 2 * HALF_TAPS), value, 0.0).astype(np.float32)
    top = value.astype(jnp.bfloat16)
    rest = (value - top.astype(np.float32)).astype(jnp.bfloat16)
    pad = np.zeros((WIDE - 3 * SPAN, WINDOW), jnp.bfloat16)
    return np.concatenate([top, top, rest, pad], axis=0)


def products(blocks):
    if blocks == 1:
        return [({0: 1}, (0,), (0,))]
    n = blocks // 2
    inner = products(n)

    def less(frames, shift):
        total = dict(frames)
        total = {m: -c for m, c in frames.items()}
        for m, c in frames.items():
            total[m + shift] = total.get(m + shift, 0) + c
        return {m: c for m, c in total.items() if c}

    both = [(f, w + tuple(i + n for i in w), o + tuple(k + n for k in o)) for f, w, o in inner]
    first = [(less(f, -n), tuple(i + n for i in w), o) for f, w, o in inner]
    last = [(less(f, n), w, tuple(k + n for k in o)) for f, w, o in inner]
    return both + first + last


def gather_kernel(
    sizes, count_ref, low_ref, mid_ref, high_ref, sl_ref, sm_ref, sh_ref, g_ref,
    recon_low, recon_mid, recon_high,
    w_out, p_full, g_out, frames_out,
    low_all, mid_all, high_all, sl_all, sm_all, sh_prev,
    low_r, mid_r, high_r, low_l, mid_l, high_l, load_sem, x_full,
    fl_top, fl_rest, fm_top, fm_rest, wm_top, wm_rest, lows, w_full,
    strain_send, strain_recv, lo_send, lf_send, lz_recv, lx_send, lx_recv, lc_send, lc_recv,
    zo_send, zf_send, z_recv, x_send, x_recv, y_send, y_recv, d_send, d_recv, c_send, c_recv,
):
    bands, peers, slices, lines, parts = sizes
    rings = peers // lines
    b, p, y = lax.axis_index("band"), lax.axis_index("tmpl"), lax.axis_index("tm")
    z, x = p // lines, p % lines
    part = y % parts

    def at_level(level):
        return (b, ((level + rings) % rings) * lines + x, y)

    def on_line(level):
        return (level >= 0) & (level < rings)

    def along_y(m):
        return (b, p, y - part + (part + m) % parts)

    across = (b, z * lines + (x + 1) % lines, y)
    sibling = (1 - b, p, y)
    before = sh_prev.shape[0]
    loads = []
    for i, (src, dst) in enumerate((
        (low_ref, low_all.at[p]), (mid_ref, mid_all.at[p]), (high_ref, high_all.at[p]),
        (sl_ref, sl_all.at[2 + y]), (sm_ref, sm_all.at[2 + y]),
        (sh_ref, x_full.at[pl.ds(before, sh_ref.shape[0])]),
        (recon_low.at[:, b, :], low_r), (recon_mid.at[:, b, :], mid_r), (recon_high.at[:, b, :], high_r),
        (g_ref, g_out),
    )):
        copy = pltpu.make_async_copy(src, dst, load_sem.at[i])
        copy.start()
        loads.append(copy)

    reach = [1, -1] if rings > 1 else []
    barrier = pltpu.get_barrier_semaphore()

    def greet(device):
        pl.semaphore_signal(barrier, inc=1, device_id=device, device_id_type=MESH)

    others = [sibling] + [(b, p, (y + k) % slices) for k in range(1, slices)]
    if lines > 1:
        others += [across]
    for device in others:
        greet(device)
    waiting = len(others)
    for step in reach:
        pl.when(on_line(z + step))(functools.partial(greet, at_level(z + step)))
        waiting = waiting + jnp.where(on_line(z + step), 1, 0)
    pl.semaphore_wait(barrier, waiting)
    for copy in loads[:6]:
        copy.wait()

    sent = []

    def remote(view, out, into, device):
        return pltpu.make_async_remote_copy(
            src_ref=view, dst_ref=view, send_sem=out, recv_sem=into, device_id=device, device_id_type=MESH
        )

    def send(view, out, into, device, when=None):
        copy = remote(view, out, into, device)
        if when is None:
            copy.start()
        else:
            pl.when(when)(copy.start)
        sent.append((copy, when))

    def arrived(view, out, into, when=None):
        copy = remote(view, out, into, sibling)
        if when is None:
            copy.wait_recv()
        else:
            pl.when(when)(copy.wait_recv)

    near = jnp.minimum(z, rings - 1 - z)
    longer = jnp.where(z < rings - 1 - z, 1, -1)
    levels = [(z, 0)]
    for n in range(1, rings):
        inside = n <= 2 * near
        step = jnp.where(inside, 1 - 2 * (n % 2), longer)
        d = jnp.where(inside, (n + 1) // 2, n - near)
        levels.append((z + step * d, step))

    arrays = (mid_all, high_all)
    size = [ref.shape[2] // (bands * parts) for ref in arrays]

    def cols(a, m=0, band=b):
        start = (band * parts + (part + m) % parts) * size[a]
        return pl.ds(pl.multiple_of(start, LANES), size[a])

    def piece(a, n, other=0, m=0, band=b):
        return arrays[a].at[levels[n][0] * lines + (x + other) % lines, :, cols(a, m, band)]

    mine = x % bands == b

    def low(n, other=0):
        return low_all.at[levels[n][0] * lines + (x + other) % lines]

    def own_low():
        for i, step in enumerate(reach):
            send(low(0), lo_send.at[i], lz_recv.at[z], at_level(z + step), mine & on_line(z + step))
        if lines > 1:
            send(low(0), lx_send.at[z], lx_recv.at[z], across, mine)

    def own_z(a):
        for i, step in enumerate(reach):
            send(piece(a, 0), zo_send.at[a, i], z_recv.at[a, z], at_level(z + step), on_line(z + step))

    def own_x(a, m):
        if lines > 1:
            send(piece(a, 0, 0, m), x_send.at[a, m, z], x_recv.at[a, m, z], across)

    def low_from_z(n):
        level, step = levels[n]
        ahead = z - step
        arrived(low(n), lf_send.at[level], lz_recv.at[level], mine)
        send(low(n), lf_send.at[level], lz_recv.at[level], at_level(ahead), mine & on_line(ahead))
        if lines > 1:
            send(low(n), lx_send.at[level], lx_recv.at[level], across, mine)
        send(low(n), lc_send.at[0, level], lc_recv.at[0, level], sibling, mine)

    def low_from_x(n):
        if lines > 1:
            level = levels[n][0]
            arrived(low(n, 1), lx_send.at[level], lx_recv.at[level], jnp.logical_not(mine))
            send(low(n, 1), lc_send.at[1, level], lc_recv.at[1, level], sibling, jnp.logical_not(mine))

    def low_landed():
        for n in range(rings):
            level = levels[n][0]
            if n > 0:
                arrived(low(n), lc_send.at[0, level], lc_recv.at[0, level], jnp.logical_not(mine))
            if lines > 1:
                arrived(low(n, 1), lc_send.at[1, level], lc_recv.at[1, level], mine)

    def pass_on(a, line, n, m, view):
        level = levels[n][0]
        send(view, c_send.at[a, line, m, level], c_recv.at[a, line, m, level], sibling)

    def from_z(a, n):
        level, step = levels[n]
        ahead = z - step
        view = piece(a, n)
        arrived(view, zf_send.at[a, level], z_recv.at[a, level])
        send(view, zf_send.at[a, level], z_recv.at[a, level], at_level(ahead), on_line(ahead))
        if lines > 1:
            send(view, x_send.at[a, 0, level], x_recv.at[a, 0, level], across)
        for m in range(1, parts):
            send(view, y_send.at[a, m, level], y_recv.at[a, m, level], along_y(m))
        pass_on(a, 0, n, 0, view)

    def from_x(a, n, m=0):
        if lines > 1:
            level = levels[n][0]
            view = piece(a, n, 1, m)
            arrived(view, x_send.at[a, m, level], x_recv.at[a, m, level])
            if n > 0 and (a, n) not in LATE_X:
                for k in range(1, parts):
                    send(view, d_send.at[a, k, level], d_recv.at[a, k, level], along_y(k))
            pass_on(a, 1, n, m, view)

    def from_y(a, n):
        level = levels[n][0]
        for m in range(1, parts):
            view = piece(a, n, 0, parts - m)
            arrived(view, y_send.at[a, m, level], y_recv.at[a, m, level])
            if lines > 1 and (a, n) in LATE_X:
                send(view, d_send.at[a, m, level], d_recv.at[a, m, level], across)
            pass_on(a, 0, n, m, view)

    def from_xy(a, n):
        if lines > 1:
            level = levels[n][0]
            for m in range(1, parts):
                view = piece(a, n, 1, parts - m)
                arrived(view, d_send.at[a, m, level], d_recv.at[a, m, level])
                pass_on(a, 1, n, m, view)

    def landed(a, own):
        for n in range(rings):
            level = levels[n][0]
            for m in range(1) if own else range(1, parts):
                if n > 0:
                    view = piece(a, n, 0, (parts - m) % parts, 1 - b)
                    arrived(view, c_send.at[a, 0, m, level], c_recv.at[a, 0, m, level])
                if lines > 1:
                    view = piece(a, n, 1, m if n == 0 else (parts - m) % parts, 1 - b)
                    arrived(view, c_send.at[a, 1, m, level], c_recv.at[a, 1, m, level])

    def blocks(a, own):
        parted = range(1) if own else range(1, parts)
        return [(cols(a, m, band), (band * parts + (part + m) % parts) * size[a]) for m in parted for band in range(bands)]

    strains = []
    for k in range(1, slices):
        device = (b, p, (y + k) % slices)
        for i, ref in enumerate((sl_all, sm_all)):
            send(ref.at[2 + y], strain_send.at[i, k], strain_recv.at[i, k], device)
            strains.append((ref.at[2 + (y + slices - k) % slices], strain_send.at[i, k], strain_recv.at[i, k]))
    if slices > 1:
        tail = pl.ds(x_full.shape[0] - before, before)
        copy = pltpu.make_async_remote_copy(
            src_ref=x_full.at[tail], dst_ref=sh_prev, send_sem=strain_send.at[2, 0], recv_sem=strain_recv.at[2, 0],
            device_id=(b, p, (y + 1) % slices), device_id_type=MESH,
        )
        copy.start()
        sent.append((copy, None))

    own_low()
    for a in range(2):
        own_z(a)
    for m in range(parts):
        for a in range(2):
            own_x(a, m)

    low_here, mid_here, low_total, mid_total = bounds(sl_ref, sm_ref, slices)
    taps_low, taps_mid = low_ref.shape[1], mid_ref.shape[1]
    low_chunks, mid_chunks = (r.shape[0] // LANES - 1 for r in (fl_top, fm_top))
    rows_mid = mid_here // LANES
    columns = p_full.shape[1]

    def low_row(r):
        return sl_all[y + 1 - taps_low // LANES + r]

    def mid_row(r):
        at = r + (y + 2) * rows_mid - taps_mid // LANES - 1
        return sm_all[at // rows_mid, pl.ds(at % rows_mid, 1), :]

    recons = ((low_r, low_l), (mid_r, mid_l), (high_r, high_l))

    def prepare(i):
        loads[6 + i].wait()
        spread_recon(*recons[i], count_ref[2 - i])

    work = [functools.partial(fill_frames, shifted(low_row, HALF_TAPS + 1), fl_top, fl_rest, low_chunks, 0, low_chunks)]
    for first in range(0, mid_chunks, 3):
        last = min(mid_chunks, first + 3)
        work += [functools.partial(fill_frames, shifted(mid_row, HALF_TAPS), fm_top, fm_rest, mid_chunks, first, last)]
    total = frames_out.shape[1]
    for block in range(frames_out.shape[0]):
        for first, last in ((0, total // 2 + 1), (total // 2 + 1, total)):
            work += [functools.partial(fill_products, x_full, frames_out, block, first, last)]

    def spend(count):
        for _ in range(count):
            if work:
                work.pop(0)()

    others = range(1, rings)
    prepare(0)
    prepare(1)
    prepare(2)
    loads[9].wait()
    for ref in (sl_all, sm_all):
        zero = jnp.zeros(ref.shape[1:], jnp.float32)
        for i in (0, 1, slices + 2, slices + 3):
            ref[i] = zero
    if slices == 1:
        sh_prev[...] = jnp.zeros(sh_prev.shape, jnp.float32)
    else:
        copy.wait_recv()
    for view in strains:
        arrived(*view)
    x_full[:before] = jnp.where(y > 0, sh_prev[...], 0.0)
    starts = range(0, columns, WIDE)

    def mid_tile(start, own):
        size_here = min(WIDE, columns - start)
        at = (mid_chunks - taps_mid // LANES - start // LANES) * LANES
        tile = slice(start, start + size_here)
        value = 0.0 if own else p_full[:, tile]
        for lanes, first in blocks(0, own):
            rows = pl.ds(pl.multiple_of(at + first, LANES), size[0])
            value += dot3((wm_top[:, lanes], wm_rest[:, lanes]), (fm_top[rows, :size_here], fm_rest[rows, :size_here]))
        if own:
            lead = start % WINDOW
            value += one_dot(lows[start // WINDOW], g_out[:, lead : lead + size_here])
        else:
            time = y * mid_here - HALF_TAPS + start + lax.broadcasted_iota(jnp.int32, value.shape, 1)
            value = jnp.where((time >= 0) & (time < mid_total), value, 0.0)
        p_full[:, tile] = value

    def mid_filters(own):
        for lanes, _ in blocks(0, own):
            wm_top[:, lanes], wm_rest[:, lanes] = split(template_filters(mid_r, mid_l, mid_all, lanes, count_ref[1]))

    def high_filters(own):
        for lanes, _ in blocks(1, own):
            w_full[:, lanes] = template_filters(high_r, high_l, high_all, lanes, count_ref[0])

    def low_part():
        low_w = split(template_filters(low_r, low_l, low_all, slice(None), count_ref[2]))
        parts_low = []
        for c in range(low_chunks):
            at = (low_chunks - 1 - c) * LANES
            parts_low.append(dot3(low_w, (fl_top[at : at + LANES, :LANES], fl_rest[at : at + LANES, :LANES])))
        value = jnp.concatenate(parts_low, axis=1)
        time = y * low_here - (HALF_TAPS + 1) + lax.broadcasted_iota(jnp.int32, value.shape, 1)
        value = jnp.where((time >= 0) & (time < low_total), value, 0.0)
        for i in range(lows.shape[0]):
            lows[i] = window(value, i * (WINDOW // RATIO))

    left = {own: list(starts) for own in (0, 1)}

    def tiles(own, count):
        for _ in range(count):
            if left[own]:
                mid_tile(left[own].pop(0), own)

    for kind, *at in ORDER:
        if kind == "f":
            spend(*at)
        elif kind == "l":
            low_landed()
            low_part()
        elif kind == "m":
            if not at[0]:
                tiles(1, len(starts))
            landed(0, *at)
            mid_filters(*at)
        elif kind == "h":
            landed(1, *at)
            high_filters(*at)
        elif kind == "t":
            tiles(*at, 1)
        else:
            a, first = at
            for n in range(first, rings if first == 3 else min(first + 1, rings)):
                if kind == "z":
                    from_z(a, n)
                elif kind == "x":
                    from_x(a, n)
                elif kind == "y":
                    from_y(a, n)
                elif kind == "d":
                    from_xy(a, n)
                else:
                    for m in range(1, parts):
                        from_x(a, 0, m)
                if a == 1 and kind == "z":
                    low_from_z(n)
                if a == 0 and kind == "x":
                    low_from_x(n)
    tiles(0, len(starts))
    spend(len(work))
    landed(1, False)
    high_filters(False)
    pieces = [w_full[:, i : i + WIDE] for i in range(0, w_full.shape[1], WIDE)]
    for i, (_, summed, _) in enumerate(products(len(pieces))):
        w_out[0, i], w_out[1, i] = split(sum(pieces[k] for k in summed))
    for copy, when in sent:
        if when is None:
            copy.wait_send()
        else:
            pl.when(when)(copy.wait_send)


def spread_recon(recon_ref, out_ref, count):
    index = lax.broadcasted_iota(jnp.int32, recon_ref.shape, 0)
    top, rest = split(jnp.where(index < count, recon_ref[...], 0.0).T)
    out_ref[...] = jnp.concatenate([top, rest, top], axis=1)


def window(value, lead):
    value = value[:, lead // LANES * LANES :][:, :WIDE]
    lead = lead % LANES
    if lead:
        value = pltpu.roll(value, WIDE - lead, 1)
    top = value.astype(jnp.bfloat16).astype(jnp.float32)
    lane = lax.broadcasted_iota(jnp.int32, value.shape, 1)
    again = jnp.where(lane < 3 * SPAN, pltpu.roll(top, 2 * SPAN, 1), 0.0)
    rest = jnp.where(lane < 2 * SPAN, pltpu.roll(value - top, SPAN, 1), again)
    return jnp.where(lane < SPAN, top, rest).astype(jnp.bfloat16)


def fill_products(x_ref, out_ref, block, first, last):
    lane = lax.broadcasted_iota(jnp.int32, (LANES, LANES), 1)
    lag = lax.broadcasted_iota(jnp.int32, (LANES, LANES), 0)
    per = WIDE // LANES
    steps = products(2 ** round(math.log(out_ref.shape[1], 3)))
    start = (block + 1) * per * len({k for _, _, outs in steps for k in outs})
    for i, (offsets, _, _) in list(enumerate(steps))[first:last]:
        before = None
        for e in range(-per, per):
            mixed = 0.0
            for m, c in offsets.items():
                row = x_ref[start + per * m + e : start + per * m + e + 1, :]
                mixed = mixed + row if c > 0 else mixed - row
            now = staggered(mixed)
            if before is not None:
                tile = split(jnp.where(lane >= lag, now, before))
                for a in range(max(0, -e), min(per, per - e)):
                    for h in range(2):
                        out_ref[block, i, h, a * LANES : (a + 1) * LANES, (a + e) * LANES : (a + e + 1) * LANES] = tile[h]
            before = now


def bounds(s_low, s_mid, slices):
    low, mid = s_low.shape[0] * LANES, s_mid.shape[0] * LANES
    return low, mid, low * slices, mid * slices


def template_filters(recon_ref, spread_ref, full, lanes, count):
    peers, rows, _ = full.shape
    if rows % 8 == 0:
        filters = full[:, :, lanes]
        top, rest = split(filters.reshape(peers * rows, filters.shape[2]))
        return one_dot(spread_ref[...], jnp.concatenate([top, top, rest], axis=0))
    first = (((0,), (0,)), ((), ()))
    index = lax.broadcasted_iota(jnp.int32, recon_ref.shape, 0)
    recon = jnp.where(index < count, recon_ref[...], 0.0)
    total = 0.0
    for p in range(peers):
        total += dot3(split(recon[p * rows : (p + 1) * rows]), split(full[p, :, lanes]), first)
    return total


def gather(sizes, count, filters, strains, g, recons):
    low, mid, high = filters
    s_low, s_mid, s_high = strains
    bands, peers, slices = sizes
    lines = 2 if peers % 2 == 0 else 1
    rings = peers // lines
    parts = math.gcd(slices, min(mid.shape[1], high.shape[1]) // (bands * LANES))
    f32, half = jnp.float32, jnp.bfloat16
    basis, _, tmpl = recons[0].shape
    taps_low, taps_mid, taps = (f.shape[1] for f in filters)
    low_here, mid_here, _, _ = bounds(s_low, s_mid, slices)
    samples = s_high.shape[0] * LANES
    columns = mid_here + LANES
    count_products = len(products(taps // WIDE))
    vmem = pl.BlockSpec(memory_space=pltpu.VMEM)
    anywhere = pl.BlockSpec(memory_space=pltpu.HBM)
    dma = pltpu.SemaphoreType.DMA

    def two(*dims):
        return [dma(dims)] * 2

    def frames(rows):
        return [pltpu.VMEM((rows, WIDE), half)] * 2

    held = [pltpu.with_memory_space_constraint(a, pltpu.HBM) for a in (count, *filters, *strains, g, *recons)]
    return pl.pallas_call(
        functools.partial(gather_kernel, (bands, peers, slices, lines, parts)),
        out_shape=[
            pltpu.VMEM((2, count_products, tmpl, WIDE), half),
            pltpu.VMEM((tmpl, columns), f32),
            pltpu.VMEM(g.shape, half),
            pltpu.VMEM((samples // taps, count_products, 2, WIDE, WIDE), half),
        ],
        in_specs=[pl.BlockSpec(memory_space=pltpu.SMEM)] + [anywhere] * 10,
        out_specs=[vmem] * 4,
        scratch_shapes=[pltpu.VMEM((peers,) + a.shape, f32) for a in filters]
        + [pltpu.VMEM((slices + 4,) + a.shape, f32) for a in (s_low, s_mid)]
        + [pltpu.VMEM((taps // LANES, LANES), f32)]
        + [pltpu.VMEM((basis, tmpl), f32)] * 3 + [pltpu.VMEM((tmpl, 3 * basis), half)] * 3
        + [dma((10,)), pltpu.VMEM(((samples + taps) // LANES, LANES), f32)]
        + frames(low_here + 2 * LANES + taps_low) + frames(columns + taps_mid)
        + [pltpu.VMEM((tmpl, taps_mid), half)] * 2
        + [pltpu.VMEM((-(-columns // WINDOW), tmpl, WIDE), half), pltpu.VMEM((tmpl, taps), f32)]
        + two(3, slices) + [dma((2,)), dma((rings,)), dma((rings,))] + two(rings) + two(2, rings)
        + [dma((2, 2)), dma((2, rings)), dma((2, rings))]
        + two(2, parts, rings) * 3 + two(2, 2, parts, rings),
        compiler_params=pltpu.CompilerParams(
            collective_id=0, has_side_effects=True, vmem_limit_bytes=28 * 1024 * 1024
        ),
        name="gather_filters",
    )(*held)


def split(value):
    top = value.astype(jnp.bfloat16)
    return top, (value - top.astype(jnp.float32)).astype(jnp.bfloat16)


def one_dot(u, v):
    return lax.dot_general(u, v, (((1,), (0,)), ((), ())), preferred_element_type=jnp.float32)


def dot3(a, b, dims=(((1,), (0,)), ((), ()))):
    def one(u, v):
        return lax.dot_general(u, v, dims, preferred_element_type=jnp.float32)

    return one(a[0], b[0]) + one(a[0], b[1]) + one(a[1], b[0])


def staggered(row):
    return pltpu.roll(jnp.broadcast_to(row, (LANES, LANES)), 0, 1, stride=1, stride_axis=0)


def shifted(read, by):
    lane = lax.broadcasted_iota(jnp.int32, (1, LANES), 1)

    def row(r):
        late = [pltpu.roll(read(r + i), by, 1) for i in range(2)]
        return jnp.where(lane >= by, late[1], late[0])

    return row


def fill_frames(row, top_ref, rest_ref, chunks, first, last):
    lane = lax.broadcasted_iota(jnp.int32, (LANES, LANES), 1)
    lag = lax.broadcasted_iota(jnp.int32, (LANES, LANES), 0)
    before = staggered(row(first))
    for c in range(first, last):
        now = staggered(row(c + 1))
        top, rest = split(jnp.where(lane >= lag, now, before))
        left, right = (chunks - 1 - c) * LANES, (chunks - c) * LANES
        for ref, value in ((top_ref, top), (rest_ref, rest)):
            ref[left : left + LANES, :LANES] = value
            ref[right : right + LANES, LANES:] = value
        before = now


def compute_kernel(strips, w_ref, p_ref, g_ref, frames_ref, out_ref, tiles, kept, spread, sems):
    rows, count = w_ref.shape[2], w_ref.shape[1]
    depth = rows // strips
    across = tiles.shape[3] // WIDE // 2

    def write(i, q, k):
        half = i % 2
        start = pl.multiple_of((2 * i + q) * (across * WIDE) + k * WIDE, WIDE)
        at = (q * across + k) * WIDE
        return pltpu.make_async_copy(
            tiles.at[half, :, :, pl.ds(at, WIDE)], out_ref.at[:, :, pl.ds(start, WIDE)], sems.at[half, q, k]
        )

    def body(*refs):
        accs = [[refs[(q * 4 + n) * strips : (q * 4 + n + 1) * strips] for n in range(4)] for q in range(2)]

        def part(r):
            return slice(r * depth, (r + 1) * depth)

        def multiply(i, n):
            for q in range(2):
                s = 2 * i + q
                acc = accs[q][n % 4]
                ends = [e for e in (4, 5, 7, 8) if e == n]
                passes = [(frames_ref.at[s, n, 0], (w_ref.at[0, n], w_ref.at[1, n]))]
                passes += [(frames_ref.at[s, n, 1], (w_ref.at[0, n],))]
                if ends:
                    k = ends_at[n]
                    lead = k * WIDE % WINDOW
                    passes += [(g_ref.at[:, lead : lead + WIDE], (spread.at[(q * across + k) * WIDE // WINDOW],))]
                for right, lefts in passes:
                    staged = turns[q] % 2
                    turns[q] += 1
                    pltpu.matmul_push_rhs(right[...], staged, q)
                    for turn, left in enumerate(lefts):
                        for r in range(strips):
                            first = staged if turn == 0 and r == 0 else None
                            pltpu.matmul_acc_lhs(acc[r], left[part(r), :], first)

        ends_at = {4: 0, 5: 1, 7: 2, 8: 3}
        turns = [0, 0]

        def finish(i, n):
            half = i % 2
            for q in range(2):
                for r in range(strips):
                    value = pltpu.matmul_pop(accs[q][n % 4][r])
                    at = (q, slice(None), part(r))
                    if n == 0:
                        kept[q, 0, part(r)] = value
                    elif n in (1, 2):
                        kept[q, n, part(r)] = kept[q, 0, part(r)] + value
                    elif n in (3, 6):
                        kept[q, 3, part(r)] = kept[q, 1, part(r)] + value
                        kept[q, 4, part(r)] = kept[q, 2, part(r)] + value
                    else:
                        k = ends_at[n]
                        at = (q * across + k) * WIDE
                        tiles[half, 0, part(r), at : at + WIDE] = kept[q, 3 + (n - 1) % 3, part(r)] + value
                if n in ends_at:
                    write(i, q, ends_at[n]).start()

        def step(i, _):
            @pl.when(i > 1)
            def _():
                for q in range(2):
                    for k in range(across):
                        write(i - 2, q, k).wait()

            stride = WINDOW // RATIO
            span = spread.shape[0] * stride
            for j in range(spread.shape[0]):
                lead = j * stride % LANES
                base = pl.multiple_of(i * span + j * stride // LANES * LANES, LANES)
                for r in range(strips):
                    spread[j, part(r)] = window(p_ref[part(r), pl.ds(base, WIDE)], lead)
            for n in range(count):
                multiply(i, n)
                if n > 0:
                    finish(i, n - 1)
            finish(i, count - 1)
            return 0

        trips = frames_ref.shape[0] // 2
        lax.fori_loop(0, trips, step, 0)
        for i in range(max(0, trips - 2), trips):
            for q in range(2):
                for k in range(across):
                    write(i, q, k).wait()

    specs = []
    for q in range(2):
        specs += [pltpu.ACC(q)((depth, WIDE), jnp.float32)] * (4 * strips)
    pl.run_scoped(body, *specs)


def compute(w, p, g, frames):
    tmpl = w.shape[2]
    blocks = len({k for _, _, outs in products(4) for k in outs})
    samples = frames.shape[0] * blocks * WIDE
    vmem = pl.BlockSpec(memory_space=pltpu.VMEM)
    return pl.pallas_call(
        functools.partial(compute_kernel, max(1, tmpl // 64)),
        out_shape=jax.ShapeDtypeStruct((1, tmpl, samples), jnp.float32),
        in_specs=[vmem] * 4,
        out_specs=pl.BlockSpec(memory_space=pltpu.HBM),
        scratch_shapes=[
            pltpu.VMEM((2, 1, tmpl, 2 * blocks * WIDE), jnp.float32),
            pltpu.VMEM((2, 5, tmpl, WIDE), jnp.float32),
            pltpu.VMEM((2 * blocks * WIDE // WINDOW, tmpl, WIDE), jnp.bfloat16),
            pltpu.SemaphoreType.DMA((2, 2, blocks)),
        ],
        compiler_params=pltpu.CompilerParams(vmem_limit_bytes=12 * 1024 * 1024),
        name="filter_templates",
    )(w, p, g, frames)


def local(
    sizes, strain_high, strain_mid, strain_low, filters_high, filters_mid, filters_low,
    recon_high, recon_mid, recon_low, basis_count,
):
    g = jnp.asarray(upsample_matrix())
    strains = [s.reshape(-1, LANES) for s in (strain_low, strain_mid, strain_high)]
    out = gather(
        sizes, basis_count, (filters_low, filters_mid, filters_high), strains, g,
        (recon_low, recon_mid, recon_high),
    )
    return compute(*out)


def solution(mesh):
    sizes = tuple(mesh.shape[name] for name in ("band", "tmpl", "tm"))
    in_specs = (
        P("tm"), P("tm"), P("tm"),
        P("tmpl", None), P("tmpl", None), P("tmpl", None),
        P(None, None, "tmpl"), P(None, None, "tmpl"), P(None, None, "tmpl"),
        P(),
    )
    return jax.shard_map(
        functools.partial(local, sizes), mesh=mesh, in_specs=in_specs,
        out_specs=P("band", "tmpl", "tm"), check_vma=False,
    )
```

```python
import functools
import math

import jax
import jax.numpy as jnp
import numpy as np
from jax import lax
from jax.experimental import pallas as pl
from jax.experimental.pallas import tpu as pltpu
from jax.sharding import PartitionSpec as P

RATIO = 8
HALF_TAPS = 8
LANES = 128
WIDE = 256
WINDOW = 2 * WIDE
SPAN = WINDOW // RATIO + 2 * HALF_TAPS
MESH = pl.DeviceIdType.MESH
ORDER = (
    ("f", 3), ("x", 0, 0), ("z", 0, 1), ("z", 0, 2), ("f", 2), ("x", 1, 0), ("z", 1, 1), ("z", 1, 2), ("f", 5),
    ("z", 0, 3), ("y", 0, 1), ("f", 3), ("z", 1, 3), ("f", 1), ("x", 0, 2), ("b", 1, 0), ("x", 0, 1), ("f", 1),
    ("y", 1, 1), ("f", 2), ("y", 1, 2), ("f", 2), ("x", 0, 3), ("f", 1), ("d", 0, 1), ("x", 1, 2), ("f", 1), ("l",),
    ("m", 1), ("y", 0, 2), ("y", 0, 3), ("x", 1, 1), ("x", 1, 3), ("t", 1), ("t", 1), ("t", 1), ("d", 0, 2),
    ("y", 1, 3), ("b", 0, 0), ("d", 0, 3), ("t", 1), ("t", 1), ("d", 1, 1), ("h", 1), ("m", 0), ("t", 0), ("d", 1, 2),
    ("d", 1, 3), ("t", 0), ("f", 1), ("t", 0), ("t", 0), ("t", 0), ("f", 1),
)
LATE_X = ((0, 1), (1, 1))


def upsample_matrix():
    u = np.arange(SPAN)[:, None]
    v = np.arange(WINDOW)[None, :]
    lag = u - v // RATIO
    offset = (v % RATIO) / RATIO - (lag - HALF_TAPS)
    value = np.sinc(offset) * (0.5 + 0.5 * np.cos(np.pi * offset / (HALF_TAPS + 1)))
    value = np.where((lag >= 0) & (lag < 2 * HALF_TAPS), value, 0.0).astype(np.float32)
    top = value.astype(jnp.bfloat16)
    rest = (value - top.astype(np.float32)).astype(jnp.bfloat16)
    pad = np.zeros((WIDE - 3 * SPAN, WINDOW), jnp.bfloat16)
    return np.concatenate([top, top, rest, pad], axis=0)


def products(blocks):
    if blocks == 1:
        return [({0: 1}, (0,), (0,))]
    n = blocks // 2
    inner = products(n)

    def less(frames, shift):
        total = dict(frames)
        total = {m: -c for m, c in frames.items()}
        for m, c in frames.items():
            total[m + shift] = total.get(m + shift, 0) + c
        return {m: c for m, c in total.items() if c}

    both = [(f, w + tuple(i + n for i in w), o + tuple(k + n for k in o)) for f, w, o in inner]
    first = [(less(f, -n), tuple(i + n for i in w), o) for f, w, o in inner]
    last = [(less(f, n), w, tuple(k + n for k in o)) for f, w, o in inner]
    return both + first + last


def gather_kernel(
    sizes, count_ref, low_ref, mid_ref, high_ref, sl_ref, sm_ref, sh_ref, g_ref,
    recon_low, recon_mid, recon_high,
    w_out, p_full, g_out, frames_out,
    low_all, mid_all, high_all, sl_all, sm_all, sh_prev,
    low_r, mid_r, high_r, low_l, mid_l, high_l, load_sem, x_full,
    fl_top, fl_rest, fm_top, fm_rest, wm_top, wm_rest, lows, w_full,
    strain_send, strain_recv, lo_send, lf_send, lz_recv, lx_send, lx_recv, lc_send, lc_recv,
    zo_send, zf_send, z_recv, x_send, x_recv, y_send, y_recv, d_send, d_recv, c_send, c_recv,
):
    bands, peers, slices, lines, parts = sizes
    rings = peers // lines
    b, p, y = lax.axis_index("band"), lax.axis_index("tmpl"), lax.axis_index("tm")
    z, x = p // lines, p % lines
    part = y % parts

    def at_level(level):
        return (b, ((level + rings) % rings) * lines + x, y)

    def on_line(level):
        return (level >= 0) & (level < rings)

    def along_y(m):
        return (b, p, y - part + (part + m) % parts)

    across = (b, z * lines + (x + 1) % lines, y)
    sibling = (1 - b, p, y)
    before = sh_prev.shape[0]
    loads = []
    for i, (src, dst) in enumerate((
        (low_ref, low_all.at[p]), (mid_ref, mid_all.at[p]), (high_ref, high_all.at[p]),
        (sl_ref, sl_all.at[2 + y]), (sm_ref, sm_all.at[2 + y]),
        (sh_ref, x_full.at[pl.ds(before, sh_ref.shape[0])]),
        (recon_low.at[:, b, :], low_r), (recon_mid.at[:, b, :], mid_r), (recon_high.at[:, b, :], high_r),
        (g_ref, g_out),
    )):
        copy = pltpu.make_async_copy(src, dst, load_sem.at[i])
        copy.start()
        loads.append(copy)

    reach = [1, -1] if rings > 1 else []
    barrier = pltpu.get_barrier_semaphore()

    def greet(device):
        pl.semaphore_signal(barrier, inc=1, device_id=device, device_id_type=MESH)

    others = [sibling] + [(b, p, (y + k) % slices) for k in range(1, slices)]
    if lines > 1:
        others += [across]
    for device in others:
        greet(device)
    waiting = len(others)
    for step in reach:
        pl.when(on_line(z + step))(functools.partial(greet, at_level(z + step)))
        waiting = waiting + jnp.where(on_line(z + step), 1, 0)
    pl.semaphore_wait(barrier, waiting)
    for copy in loads[:6]:
        copy.wait()

    sent = []

    def remote(view, out, into, device):
        return pltpu.make_async_remote_copy(
            src_ref=view, dst_ref=view, send_sem=out, recv_sem=into, device_id=device, device_id_type=MESH
        )

    def send(view, out, into, device, when=None):
        copy = remote(view, out, into, device)
        if when is None:
            copy.start()
        else:
            pl.when(when)(copy.start)
        sent.append((copy, when))

    def arrived(view, out, into, when=None):
        copy = remote(view, out, into, sibling)
        if when is None:
            copy.wait_recv()
        else:
            pl.when(when)(copy.wait_recv)

    near = jnp.minimum(z, rings - 1 - z)
    longer = jnp.where(z < rings - 1 - z, 1, -1)
    levels = [(z, 0)]
    for n in range(1, rings):
        inside = n <= 2 * near
        step = jnp.where(inside, 1 - 2 * (n % 2), longer)
        d = jnp.where(inside, (n + 1) // 2, n - near)
        levels.append((z + step * d, step))

    arrays = (mid_all, high_all)
    size = [ref.shape[2] // (bands * parts) for ref in arrays]

    def cols(a, m=0, band=b):
        start = (band * parts + (part + m) % parts) * size[a]
        return pl.ds(pl.multiple_of(start, LANES), size[a])

    def piece(a, n, other=0, m=0, band=b):
        return arrays[a].at[levels[n][0] * lines + (x + other) % lines, :, cols(a, m, band)]

    mine = x % bands == b

    def low(n, other=0):
        return low_all.at[levels[n][0] * lines + (x + other) % lines]

    def own_low():
        for i, step in enumerate(reach):
            send(low(0), lo_send.at[i], lz_recv.at[z], at_level(z + step), mine & on_line(z + step))
        if lines > 1:
            send(low(0), lx_send.at[z], lx_recv.at[z], across, mine)

    def own_z(a):
        for i, step in enumerate(reach):
            send(piece(a, 0), zo_send.at[a, i], z_recv.at[a, z], at_level(z + step), on_line(z + step))

    def own_x(a, m):
        if lines > 1:
            send(piece(a, 0, 0, m), x_send.at[a, m, z], x_recv.at[a, m, z], across)

    def low_from_z(n):
        level, step = levels[n]
        ahead = z - step
        arrived(low(n), lf_send.at[level], lz_recv.at[level], mine)
        send(low(n), lf_send.at[level], lz_recv.at[level], at_level(ahead), mine & on_line(ahead))
        if lines > 1:
            send(low(n), lx_send.at[level], lx_recv.at[level], across, mine)
        send(low(n), lc_send.at[0, level], lc_recv.at[0, level], sibling, mine)

    def low_from_x(n):
        if lines > 1:
            level = levels[n][0]
            arrived(low(n, 1), lx_send.at[level], lx_recv.at[level], jnp.logical_not(mine))
            send(low(n, 1), lc_send.at[1, level], lc_recv.at[1, level], sibling, jnp.logical_not(mine))

    def low_landed():
        for n in range(rings):
            level = levels[n][0]
            if n > 0:
                arrived(low(n), lc_send.at[0, level], lc_recv.at[0, level], jnp.logical_not(mine))
            if lines > 1:
                arrived(low(n, 1), lc_send.at[1, level], lc_recv.at[1, level], mine)

    def pass_on(a, line, n, m, view):
        level = levels[n][0]
        send(view, c_send.at[a, line, m, level], c_recv.at[a, line, m, level], sibling)

    def from_z(a, n):
        level, step = levels[n]
        ahead = z - step
        view = piece(a, n)
        arrived(view, zf_send.at[a, level], z_recv.at[a, level])
        send(view, zf_send.at[a, level], z_recv.at[a, level], at_level(ahead), on_line(ahead))
        if lines > 1:
            send(view, x_send.at[a, 0, level], x_recv.at[a, 0, level], across)
        for m in range(1, parts):
            send(view, y_send.at[a, m, level], y_recv.at[a, m, level], along_y(m))
        pass_on(a, 0, n, 0, view)

    def from_x(a, n, m=0):
        if lines > 1:
            level = levels[n][0]
            view = piece(a, n, 1, m)
            arrived(view, x_send.at[a, m, level], x_recv.at[a, m, level])
            if n > 0 and (a, n) not in LATE_X:
                for k in range(1, parts):
                    send(view, d_send.at[a, k, level], d_recv.at[a, k, level], along_y(k))
            pass_on(a, 1, n, m, view)

    def from_y(a, n):
        level = levels[n][0]
        for m in range(1, parts):
            view = piece(a, n, 0, parts - m)
            arrived(view, y_send.at[a, m, level], y_recv.at[a, m, level])
            if lines > 1 and (a, n) in LATE_X:
                send(view, d_send.at[a, m, level], d_recv.at[a, m, level], across)
            pass_on(a, 0, n, m, view)

    def from_xy(a, n):
        if lines > 1:
            level = levels[n][0]
            for m in range(1, parts):
                view = piece(a, n, 1, parts - m)
                arrived(view, d_send.at[a, m, level], d_recv.at[a, m, level])
                pass_on(a, 1, n, m, view)

    def landed(a, own):
        for n in range(rings):
            level = levels[n][0]
            for m in range(1) if own else range(1, parts):
                if n > 0:
                    view = piece(a, n, 0, (parts - m) % parts, 1 - b)
                    arrived(view, c_send.at[a, 0, m, level], c_recv.at[a, 0, m, level])
                if lines > 1:
                    view = piece(a, n, 1, m if n == 0 else (parts - m) % parts, 1 - b)
                    arrived(view, c_send.at[a, 1, m, level], c_recv.at[a, 1, m, level])

    def blocks(a, own):
        parted = range(1) if own else range(1, parts)
        return [(cols(a, m, band), (band * parts + (part + m) % parts) * size[a]) for m in parted for band in range(bands)]

    strains = []
    for k in range(1, slices):
        device = (b, p, (y + k) % slices)
        for i, ref in enumerate((sl_all, sm_all)):
            send(ref.at[2 + y], strain_send.at[i, k], strain_recv.at[i, k], device)
            strains.append((ref.at[2 + (y + slices - k) % slices], strain_send.at[i, k], strain_recv.at[i, k]))
    if slices > 1:
        tail = pl.ds(x_full.shape[0] - before, before)
        copy = pltpu.make_async_remote_copy(
            src_ref=x_full.at[tail], dst_ref=sh_prev, send_sem=strain_send.at[2, 0], recv_sem=strain_recv.at[2, 0],
            device_id=(b, p, (y + 1) % slices), device_id_type=MESH,
        )
        copy.start()
        sent.append((copy, None))

    own_low()
    for a in range(2):
        own_z(a)
    for m in range(parts):
        for a in range(2):
            own_x(a, m)

    low_here, mid_here, low_total, mid_total = bounds(sl_ref, sm_ref, slices)
    taps_low, taps_mid = low_ref.shape[1], mid_ref.shape[1]
    low_chunks, mid_chunks = (r.shape[0] // LANES - 1 for r in (fl_top, fm_top))
    rows_mid = mid_here // LANES
    columns = p_full.shape[1]

    def low_row(r):
        return sl_all[y + 1 - taps_low // LANES + r]

    def mid_row(r):
        at = r + (y + 2) * rows_mid - taps_mid // LANES - 1
        return sm_all[at // rows_mid, pl.ds(at % rows_mid, 1), :]

    recons = ((low_r, low_l), (mid_r, mid_l), (high_r, high_l))

    def prepare(i):
        loads[6 + i].wait()
        spread_recon(*recons[i], count_ref[2 - i])

    work = [functools.partial(fill_frames, shifted(low_row, HALF_TAPS + 1), fl_top, fl_rest, low_chunks, 0, low_chunks)]
    for first in range(0, mid_chunks, 3):
        last = min(mid_chunks, first + 3)
        work += [functools.partial(fill_frames, shifted(mid_row, HALF_TAPS), fm_top, fm_rest, mid_chunks, first, last)]
    total = frames_out.shape[1]
    for block in range(frames_out.shape[0]):
        for first, last in ((0, total // 2 + 1), (total // 2 + 1, total)):
            work += [functools.partial(fill_products, x_full, frames_out, block, first, last)]

    def spend(count):
        for _ in range(count):
            if work:
                work.pop(0)()

    others = range(1, rings)
    prepare(0)
    prepare(1)
    prepare(2)
    loads[9].wait()
    for ref in (sl_all, sm_all):
        zero = jnp.zeros(ref.shape[1:], jnp.float32)
        for i in (0, 1, slices + 2, slices + 3):
            ref[i] = zero
    if slices == 1:
        sh_prev[...] = jnp.zeros(sh_prev.shape, jnp.float32)
    else:
        copy.wait_recv()
    for view in strains:
        arrived(*view)
    x_full[:before] = jnp.where(y > 0, sh_prev[...], 0.0)
    starts = range(0, columns, WIDE)

    def mid_tile(start, own):
        size_here = min(WIDE, columns - start)
        at = (mid_chunks - taps_mid // LANES - start // LANES) * LANES
        tile = slice(start, start + size_here)
        value = 0.0 if own else p_full[:, tile]
        for lanes, first in blocks(0, own):
            rows = pl.ds(pl.multiple_of(at + first, LANES), size[0])
            value += dot3((wm_top[:, lanes], wm_rest[:, lanes]), (fm_top[rows, :size_here], fm_rest[rows, :size_here]))
        if own:
            lead = start % WINDOW
            value += one_dot(lows[start // WINDOW], g_out[:, lead : lead + size_here])
        else:
            time = y * mid_here - HALF_TAPS + start + lax.broadcasted_iota(jnp.int32, value.shape, 1)
            value = jnp.where((time >= 0) & (time < mid_total), value, 0.0)
        p_full[:, tile] = value

    def mid_filters(own):
        for lanes, _ in blocks(0, own):
            wm_top[:, lanes], wm_rest[:, lanes] = split(template_filters(mid_r, mid_l, mid_all, lanes, count_ref[1]))

    def high_filters(own):
        for lanes, _ in blocks(1, own):
            w_full[:, lanes] = template_filters(high_r, high_l, high_all, lanes, count_ref[0])

    def low_part():
        low_w = split(template_filters(low_r, low_l, low_all, slice(None), count_ref[2]))
        parts_low = []
        for c in range(low_chunks):
            at = (low_chunks - 1 - c) * LANES
            parts_low.append(dot3(low_w, (fl_top[at : at + LANES, :LANES], fl_rest[at : at + LANES, :LANES])))
        value = jnp.concatenate(parts_low, axis=1)
        time = y * low_here - (HALF_TAPS + 1) + lax.broadcasted_iota(jnp.int32, value.shape, 1)
        value = jnp.where((time >= 0) & (time < low_total), value, 0.0)
        for i in range(lows.shape[0]):
            lows[i] = window(value, i * (WINDOW // RATIO))

    left = {own: list(starts) for own in (0, 1)}

    def tiles(own, count):
        for _ in range(count):
            if left[own]:
                mid_tile(left[own].pop(0), own)

    for kind, *at in ORDER:
        if kind == "f":
            spend(*at)
        elif kind == "l":
            low_landed()
            low_part()
        elif kind == "m":
            if not at[0]:
                tiles(1, len(starts))
            landed(0, *at)
            mid_filters(*at)
        elif kind == "h":
            landed(1, *at)
            high_filters(*at)
        elif kind == "t":
            tiles(*at, 1)
        else:
            a, first = at
            for n in range(first, rings if first == 3 else min(first + 1, rings)):
                if kind == "z":
                    from_z(a, n)
                elif kind == "x":
                    from_x(a, n)
                elif kind == "y":
                    from_y(a, n)
                elif kind == "d":
                    from_xy(a, n)
                else:
                    for m in range(1, parts):
                        from_x(a, 0, m)
                if a == 1 and kind == "z":
                    low_from_z(n)
                if a == 0 and kind == "x":
                    low_from_x(n)
    tiles(0, len(starts))
    spend(len(work))
    landed(1, False)
    high_filters(False)
    pieces = [w_full[:, i : i + WIDE] for i in range(0, w_full.shape[1], WIDE)]
    for i, (_, summed, _) in enumerate(products(len(pieces))):
        w_out[0, i], w_out[1, i] = split(sum(pieces[k] for k in summed))
    for copy, when in sent:
        if when is None:
            copy.wait_send()
        else:
            pl.when(when)(copy.wait_send)


def spread_recon(recon_ref, out_ref, count):
    index = lax.broadcasted_iota(jnp.int32, recon_ref.shape, 0)
    top, rest = split(jnp.where(index < count, recon_ref[...], 0.0).T)
    out_ref[...] = jnp.concatenate([top, rest, top], axis=1)


def window(value, lead):
    value = value[:, lead // LANES * LANES :][:, :WIDE]
    lead = lead % LANES
    if lead:
        value = pltpu.roll(value, WIDE - lead, 1)
    top = value.astype(jnp.bfloat16).astype(jnp.float32)
    lane = lax.broadcasted_iota(jnp.int32, value.shape, 1)
    again = jnp.where(lane < 3 * SPAN, pltpu.roll(top, 2 * SPAN, 1), 0.0)
    rest = jnp.where(lane < 2 * SPAN, pltpu.roll(value - top, SPAN, 1), again)
    return jnp.where(lane < SPAN, top, rest).astype(jnp.bfloat16)


def fill_products(x_ref, out_ref, block, first, last):
    lane = lax.broadcasted_iota(jnp.int32, (LANES, LANES), 1)
    lag = lax.broadcasted_iota(jnp.int32, (LANES, LANES), 0)
    per = WIDE // LANES
    steps = products(2 ** round(math.log(out_ref.shape[1], 3)))
    start = (block + 1) * per * len({k for _, _, outs in steps for k in outs})
    for i, (offsets, _, _) in list(enumerate(steps))[first:last]:
        before = None
        for e in range(-per, per):
            mixed = 0.0
            for m, c in offsets.items():
                row = x_ref[start + per * m + e : start + per * m + e + 1, :]
                mixed = mixed + row if c > 0 else mixed - row
            now = staggered(mixed)
            if before is not None:
                tile = split(jnp.where(lane >= lag, now, before))
                for a in range(max(0, -e), min(per, per - e)):
                    for h in range(2):
                        out_ref[block, i, h, a * LANES : (a + 1) * LANES, (a + e) * LANES : (a + e + 1) * LANES] = tile[h]
            before = now


def bounds(s_low, s_mid, slices):
    low, mid = s_low.shape[0] * LANES, s_mid.shape[0] * LANES
    return low, mid, low * slices, mid * slices


def template_filters(recon_ref, spread_ref, full, lanes, count):
    peers, rows, _ = full.shape
    if rows % 8 == 0:
        filters = full[:, :, lanes]
        top, rest = split(filters.reshape(peers * rows, filters.shape[2]))
        return one_dot(spread_ref[...], jnp.concatenate([top, top, rest], axis=0))
    first = (((0,), (0,)), ((), ()))
    index = lax.broadcasted_iota(jnp.int32, recon_ref.shape, 0)
    recon = jnp.where(index < count, recon_ref[...], 0.0)
    total = 0.0
    for p in range(peers):
        total += dot3(split(recon[p * rows : (p + 1) * rows]), split(full[p, :, lanes]), first)
    return total


def gather(sizes, count, filters, strains, g, recons):
    low, mid, high = filters
    s_low, s_mid, s_high = strains
    bands, peers, slices = sizes
    lines = 2 if peers % 2 == 0 else 1
    rings = peers // lines
    parts = math.gcd(slices, min(mid.shape[1], high.shape[1]) // (bands * LANES))
    f32, half = jnp.float32, jnp.bfloat16
    basis, _, tmpl = recons[0].shape
    taps_low, taps_mid, taps = (f.shape[1] for f in filters)
    low_here, mid_here, _, _ = bounds(s_low, s_mid, slices)
    samples = s_high.shape[0] * LANES
    columns = mid_here + LANES
    count_products = len(products(taps // WIDE))
    vmem = pl.BlockSpec(memory_space=pltpu.VMEM)
    anywhere = pl.BlockSpec(memory_space=pltpu.HBM)
    dma = pltpu.SemaphoreType.DMA

    def two(*dims):
        return [dma(dims)] * 2

    def frames(rows):
        return [pltpu.VMEM((rows, WIDE), half)] * 2

    held = [pltpu.with_memory_space_constraint(a, pltpu.HBM) for a in (count, *filters, *strains, g, *recons)]
    return pl.pallas_call(
        functools.partial(gather_kernel, (bands, peers, slices, lines, parts)),
        out_shape=[
            pltpu.VMEM((2, count_products, tmpl, WIDE), half),
            pltpu.VMEM((tmpl, columns), f32),
            pltpu.VMEM(g.shape, half),
            pltpu.VMEM((samples // taps, count_products, 2, WIDE, WIDE), half),
        ],
        in_specs=[pl.BlockSpec(memory_space=pltpu.SMEM)] + [anywhere] * 10,
        out_specs=[vmem] * 4,
        scratch_shapes=[pltpu.VMEM((peers,) + a.shape, f32) for a in filters]
        + [pltpu.VMEM((slices + 4,) + a.shape, f32) for a in (s_low, s_mid)]
        + [pltpu.VMEM((taps // LANES, LANES), f32)]
        + [pltpu.VMEM((basis, tmpl), f32)] * 3 + [pltpu.VMEM((tmpl, 3 * basis), half)] * 3
        + [dma((10,)), pltpu.VMEM(((samples + taps) // LANES, LANES), f32)]
        + frames(low_here + 2 * LANES + taps_low) + frames(columns + taps_mid)
        + [pltpu.VMEM((tmpl, taps_mid), half)] * 2
        + [pltpu.VMEM((-(-columns // WINDOW), tmpl, WIDE), half), pltpu.VMEM((tmpl, taps), f32)]
        + two(3, slices) + [dma((2,)), dma((rings,)), dma((rings,))] + two(rings) + two(2, rings)
        + [dma((2, 2)), dma((2, rings)), dma((2, rings))]
        + two(2, parts, rings) * 3 + two(2, 2, parts, rings),
        compiler_params=pltpu.CompilerParams(
            collective_id=0, has_side_effects=True, vmem_limit_bytes=28 * 1024 * 1024
        ),
        name="gather_filters",
    )(*held)


def split(value):
    top = value.astype(jnp.bfloat16)
    return top, (value - top.astype(jnp.float32)).astype(jnp.bfloat16)


def one_dot(u, v):
    return lax.dot_general(u, v, (((1,), (0,)), ((), ())), preferred_element_type=jnp.float32)


def dot3(a, b, dims=(((1,), (0,)), ((), ()))):
    def one(u, v):
        return lax.dot_general(u, v, dims, preferred_element_type=jnp.float32)

    return one(a[0], b[0]) + one(a[0], b[1]) + one(a[1], b[0])


def staggered(row):
    return pltpu.roll(jnp.broadcast_to(row, (LANES, LANES)), 0, 1, stride=1, stride_axis=0)


def shifted(read, by):
    lane = lax.broadcasted_iota(jnp.int32, (1, LANES), 1)

    def row(r):
        late = [pltpu.roll(read(r + i), by, 1) for i in range(2)]
        return jnp.where(lane >= by, late[1], late[0])

    return row


def fill_frames(row, top_ref, rest_ref, chunks, first, last):
    lane = lax.broadcasted_iota(jnp.int32, (LANES, LANES), 1)
    lag = lax.broadcasted_iota(jnp.int32, (LANES, LANES), 0)
    before = staggered(row(first))
    for c in range(first, last):
        now = staggered(row(c + 1))
        top, rest = split(jnp.where(lane >= lag, now, before))
        left, right = (chunks - 1 - c) * LANES, (chunks - c) * LANES
        for ref, value in ((top_ref, top), (rest_ref, rest)):
            ref[left : left + LANES, :LANES] = value
            ref[right : right + LANES, LANES:] = value
        before = now


def compute_kernel(strips, w_ref, p_ref, g_ref, frames_ref, out_ref, tiles, kept, spread, sems):
    rows, count = w_ref.shape[2], w_ref.shape[1]
    depth = rows // strips
    across = tiles.shape[3] // WIDE // 2

    def write(i, q, k):
        half = i % 2
        start = pl.multiple_of((2 * i + q) * (across * WIDE) + k * WIDE, WIDE)
        at = (q * across + k) * WIDE
        return pltpu.make_async_copy(
            tiles.at[half, :, :, pl.ds(at, WIDE)], out_ref.at[:, :, pl.ds(start, WIDE)], sems.at[half, q, k]
        )

    def body(*refs):
        accs = [[refs[(q * 4 + n) * strips : (q * 4 + n + 1) * strips] for n in range(4)] for q in range(2)]

        def part(r):
            return slice(r * depth, (r + 1) * depth)

        def multiply(i, n):
            for q in range(2):
                s = 2 * i + q
                acc = accs[q][n % 4]
                ends = [e for e in (4, 5, 7, 8) if e == n]
                passes = [(frames_ref.at[s, n, 0], (w_ref.at[0, n], w_ref.at[1, n]))]
                passes += [(frames_ref.at[s, n, 1], (w_ref.at[0, n],))]
                if ends:
                    k = ends_at[n]
                    lead = k * WIDE % WINDOW
                    passes += [(g_ref.at[:, lead : lead + WIDE], (spread.at[(q * across + k) * WIDE // WINDOW],))]
                for right, lefts in passes:
                    staged = turns[q] % 2
                    turns[q] += 1
                    pltpu.matmul_push_rhs(right[...], staged, q)
                    for turn, left in enumerate(lefts):
                        for r in range(strips):
                            first = staged if turn == 0 and r == 0 else None
                            pltpu.matmul_acc_lhs(acc[r], left[part(r), :], first)

        ends_at = {4: 0, 5: 1, 7: 2, 8: 3}
        turns = [0, 0]

        def finish(i, n):
            half = i % 2
            for q in range(2):
                for r in range(strips):
                    value = pltpu.matmul_pop(accs[q][n % 4][r])
                    at = (q, slice(None), part(r))
                    if n == 0:
                        kept[q, 0, part(r)] = value
                    elif n in (1, 2):
                        kept[q, n, part(r)] = kept[q, 0, part(r)] + value
                    elif n in (3, 6):
                        kept[q, 3, part(r)] = kept[q, 1, part(r)] + value
                        kept[q, 4, part(r)] = kept[q, 2, part(r)] + value
                    else:
                        k = ends_at[n]
                        at = (q * across + k) * WIDE
                        tiles[half, 0, part(r), at : at + WIDE] = kept[q, 3 + (n - 1) % 3, part(r)] + value
                if n in ends_at:
                    write(i, q, ends_at[n]).start()

        def step(i, _):
            @pl.when(i > 1)
            def _():
                for q in range(2):
                    for k in range(across):
                        write(i - 2, q, k).wait()

            stride = WINDOW // RATIO
            span = spread.shape[0] * stride
            for j in range(spread.shape[0]):
                lead = j * stride % LANES
                base = pl.multiple_of(i * span + j * stride // LANES * LANES, LANES)
                for r in range(strips):
                    spread[j, part(r)] = window(p_ref[part(r), pl.ds(base, WIDE)], lead)
            for n in range(count):
                multiply(i, n)
                if n > 0:
                    finish(i, n - 1)
            finish(i, count - 1)
            return 0

        trips = frames_ref.shape[0] // 2
        lax.fori_loop(0, trips, step, 0)
        for i in range(max(0, trips - 2), trips):
            for q in range(2):
                for k in range(across):
                    write(i, q, k).wait()

    specs = []
    for q in range(2):
        specs += [pltpu.ACC(q)((depth, WIDE), jnp.float32)] * (4 * strips)
    pl.run_scoped(body, *specs)


def compute(w, p, g, frames):
    tmpl = w.shape[2]
    blocks = len({k for _, _, outs in products(4) for k in outs})
    samples = frames.shape[0] * blocks * WIDE
    vmem = pl.BlockSpec(memory_space=pltpu.VMEM)
    return pl.pallas_call(
        functools.partial(compute_kernel, max(1, tmpl // 64)),
        out_shape=jax.ShapeDtypeStruct((1, tmpl, samples), jnp.float32),
        in_specs=[vmem] * 4,
        out_specs=pl.BlockSpec(memory_space=pltpu.HBM),
        scratch_shapes=[
            pltpu.VMEM((2, 1, tmpl, 2 * blocks * WIDE), jnp.float32),
            pltpu.VMEM((2, 5, tmpl, WIDE), jnp.float32),
            pltpu.VMEM((2 * blocks * WIDE // WINDOW, tmpl, WIDE), jnp.bfloat16),
            pltpu.SemaphoreType.DMA((2, 2, blocks)),
        ],
        compiler_params=pltpu.CompilerParams(vmem_limit_bytes=12 * 1024 * 1024),
        name="filter_templates",
    )(w, p, g, frames)


def local(
    sizes, strain_high, strain_mid, strain_low, filters_high, filters_mid, filters_low,
    recon_high, recon_mid, recon_low, basis_count,
):
    g = jnp.asarray(upsample_matrix())
    strains = [s.reshape(-1, LANES) for s in (strain_low, strain_mid, strain_high)]
    out = gather(
        sizes, basis_count, (filters_low, filters_mid, filters_high), strains, g,
        (recon_low, recon_mid, recon_high),
    )
    return compute(*out)


def solution(mesh):
    sizes = tuple(mesh.shape[name] for name in ("band", "tmpl", "tm"))
    in_specs = (
        P("tm"), P("tm"), P("tm"),
        P("tmpl", None), P("tmpl", None), P("tmpl", None),
        P(None, None, "tmpl"), P(None, None, "tmpl"), P(None, None, "tmpl"),
        P(),
    )
    return jax.shard_map(
        functools.partial(local, sizes), mesh=mesh, in_specs=in_specs,
        out_specs=P("band", "tmpl", "tm"), check_vma=False,
    )
```
